32 devices in a mesh: gx: 4 (over y, x), gy: 8 (over z, core).
Axes of the slice: x: 2, y: 2, z: 4, core: 2. Of those that a mesh axis runs over, the one named last changes fastest.
Arguments:
- tile_flux: bfloat16 [4, 12, 8, 131072], P(None, None, None, ('gx', 'gy')), may hold values from -6 to 6
- tile_frac: float32 [8, 131072], P(None, ('gx', 'gy')), may hold values from 0.02 to 1
- weights: bfloat16 [32, 7, 16, 256, 128], P(('gx', 'gy')), may hold values from -0.049804688 to 0.14941406
- block_row: int32 [32, 7, 16], P(('gx', 'gy')), may hold values from 0 to 47
- block_col: int32 [32, 7, 16], P(('gx', 'gy')), may hold values from 0 to 31
- send_counts: int32 [32, 7], P(('gx', 'gy')), may hold values from 1 to 16, as said below
Outputs:
- atm_flux: float32 [4, 12, 393216], P(None, None, ('gx', 'gy'))
The draws below stay inside these ranges and needn't reach their ends.
Inputs may be any that keep to these rules, and one draw needn't show every extreme that they name: `send_counts`: live slots of a device at an offset; some device has all 7 offsets at 16, and some device receives 16 live slots from every offset.
All inputs are finite; a program needn't handle non-finite values.
Results may differ from the reference program's by a relative error of at most 0.0029.
Values sent between devices are 32-bit elements; how exact they have to be, the bound alone decides.
A program may use at most 128 MiB of HBM per device.

```python
import math
import jax
import jax.numpy as jnp
from jax import lax

NFLUX = 12
TILES = 8
SUBSTEPS = 4
BROWS = 256
LCOLS = 128
REACH = 3
CAP = 16
LB_DEV = 32
AB_DEV = 48
NOFF = 7
LAND_CELLS = 131072
ATM_CELLS = 393216
DEVICES = 32


def draw_send_counts(key, part):
    key_base, key_full = jax.random.split(jax.random.fold_in(key, 17))
    base = jax.random.randint(key_base, (DEVICES, NOFF), 1, CAP // 2 + 1)
    full_dev = jax.random.randint(key_full, (), 0, DEVICES)
    row_ids = jnp.arange(DEVICES, dtype=jnp.int32)[:, None]
    col_ids = jnp.arange(NOFF, dtype=jnp.int32)[None, :]
    source = (full_dev - (col_ids - REACH)) % DEVICES
    filled = (row_ids == full_dev) | (row_ids == source)
    return jnp.where(filled, CAP, base).astype(jnp.int32)


def plant(values, key, least, top_value):
    spot = [jax.random.randint(jax.random.fold_in(key, axis), (), 0, length) for axis, length in enumerate(values.shape)]
    widest = values.shape.index(max(values.shape))
    next_to = spot[:widest] + [(spot[widest] + 1) % values.shape[widest]] + spot[widest + 1:]
    return values.at[tuple(spot)].set(least).at[tuple(next_to)].set(top_value)


def block_scale(own_key, extent, cuts, low, high):
    factor_of = 1.0
    for axis_at, shards_of in cuts:
        steps = jax.random.uniform(jax.random.fold_in(jax.random.fold_in(own_key, 6), axis_at), (shards_of,), jnp.float32, low / len(cuts), high / len(cuts))
        factor_of = factor_of * jnp.repeat(jnp.exp(steps), extent[axis_at] // shards_of).reshape((-1,) + (1,) * (len(extent) - 1 - axis_at))
    return factor_of


def bell_draw(stream_key, extent, spread, bound, cuts=(), held_as=jnp.bfloat16):
    result = spread * jax.random.normal(stream_key, extent, jnp.float32)
    if cuts:
        result = result * block_scale(stream_key, extent, cuts, -0.22, 0.18)
    return jnp.clip(result, -bound, bound).astype(held_as)


def setup_inputs(seed: int = 0) -> dict:
    streams_of = jax.random.split(jax.random.key(seed), 7)
    tile_flux = bell_draw(streams_of[0], (SUBSTEPS, NFLUX, TILES, LAND_CELLS), 1.0, 6.0, ((3, 32),))
    tile_frac = jnp.clip(jnp.exp(math.log(1.0) - 3.912023 * jax.random.uniform(streams_of[1], (TILES, LAND_CELLS), jnp.float32) ** block_scale(streams_of[1], (TILES, LAND_CELLS), ((1, 32),), -0.2, 0.2)), 0.02, 1.0)
    weights = jnp.clip(-0.049804688 + 0.19921875 * jax.random.uniform(streams_of[2], (DEVICES, NOFF, CAP, BROWS, LCOLS), jnp.float32) ** block_scale(streams_of[2], (DEVICES, NOFF, CAP, BROWS, LCOLS), ((0, 32),), -0.2, 0.2), -0.049804688, 0.14941406).astype(jnp.bfloat16)
    block_row = plant(jax.random.randint(streams_of[3], (DEVICES, NOFF, CAP), 0, AB_DEV), jax.random.fold_in(streams_of[3], 1), 0, AB_DEV - 1).astype(jnp.int32)
    block_col = plant(jax.random.randint(streams_of[4], (DEVICES, NOFF, CAP), 0, LB_DEV), jax.random.fold_in(streams_of[4], 1), 0, LB_DEV - 1).astype(jnp.int32)
    send_counts = draw_send_counts(jax.random.fold_in(streams_of[6], 71), 0)
    return {"tile_flux": tile_flux, "tile_frac": tile_frac, "weights": weights, "block_row": block_row, "block_col": block_col, "send_counts": send_counts}


def reference(tile_flux, tile_frac, weights, block_row, block_col, send_counts):
    frac_sum = jnp.sum(tile_frac, axis=0)
    merged = (jnp.sum(tile_flux.astype(jnp.float32) * tile_frac[None, None], axis=2) / frac_sum).astype(jnp.bfloat16)
    width = SUBSTEPS * NFLUX
    land_blocks = merged.reshape(width, DEVICES, LB_DEV, LCOLS).transpose(1, 2, 0, 3)

    def one_device(block_w, columns, counts, blocks):
        picked = blocks[columns]
        partial_value = jnp.einsum('okrc,okfc->okfr', block_w.astype(jnp.float32), picked.astype(jnp.float32))
        active = (jnp.arange(CAP, dtype=jnp.int32)[None, :] < counts[:, None]).astype(jnp.float32)
        return partial_value * active[:, :, None, None]

    def one_group(items):
        return jax.vmap(one_device)(*items)

    group = 8
    grouped = (weights.reshape((DEVICES // group, group) + weights.shape[1:]),
               block_col.reshape((DEVICES // group, group) + block_col.shape[1:]),
               send_counts.reshape((DEVICES // group, group) + send_counts.shape[1:]),
               land_blocks.reshape((DEVICES // group, group) + land_blocks.shape[1:]))
    partials = lax.map(one_group, grouped)
    dest_dev = (jnp.arange(DEVICES, dtype=jnp.int32)[:, None] + jnp.arange(NOFF, dtype=jnp.int32)[None, :] - REACH) % DEVICES
    target = (dest_dev[:, :, None] * AB_DEV + block_row).astype(jnp.int32)
    totals = jnp.zeros((DEVICES * AB_DEV, width, BROWS), jnp.float32)
    totals = totals.at[target.reshape(-1)].add(partials.reshape(-1, width, BROWS))
    return totals.transpose(1, 0, 2).reshape(SUBSTEPS, NFLUX, ATM_CELLS)
```

```python
import functools

import jax
import jax.numpy as jnp
from jax import lax
from jax.experimental import pallas as pl
from jax.experimental.pallas import tpu as pltpu
from jax.sharding import PartitionSpec as P

OUT_CUTS = 4
EARLY = 4
CLASSES = 16
LANES = 128
COUNT_LANE = 64
AB_DEV = 48


def ranges(begin, end, sizes):
    spans = []
    for size in sizes:
        size = min(size, end - begin)
        if size > 0:
            spans.append((begin, size))
            begin += size
    if begin < end:
        spans.append((begin, end - begin))
    return spans


def flow_order(reach):
    order = []
    for away in range(reach, 0, -1):
        order += [reach + away, reach - away]
    return order


def greet(me, count, place):
    barrier = pltpu.get_barrier_semaphore()

    def one(step, carry):
        pl.semaphore_signal(barrier, inc=1, device_id=place(lax.rem(me + step, count)),
                            device_id_type=pl.DeviceIdType.MESH)
        return carry

    lax.fori_loop(1, count, one, 0)
    return barrier


def exchange_kernel(axes, sizes, first, half, flux_ref, frac_ref, col_ref, count_ref, rows_ref,
                    weights_ref, part_ref, own_ref, arrived_ref, arrived_rows_ref, votes_ref,
                    pick_ref,
                    flux_buf, frac_buf, weights_buf, flux_sem, frac_sem, weight_sem,
                    own_sem, send_sem, recv_sem, row_send_sem, row_recv_sem,
                    vote_send_sem, vote_recv_sem):
    num_off, slots = weights_buf.shape[0], weights_buf.shape[1]
    num_steps, num_kinds, tiles, _ = flux_ref.shape
    cols = weights_buf.shape[3]
    reach = num_off // 2
    inner = sizes[1]
    count = sizes[0] * sizes[1]
    me = lax.axis_index(axes[0]) * inner + lax.axis_index(axes[1])
    first_spans = ranges(0, first, (1, 1, 2))
    later_spans = ranges(first, slots, (half - first,))

    def place(there):
        return (there // inner, lax.rem(there, inner))

    def target(offset):
        return lax.rem(me + offset - reach + count, count)

    barrier = greet(me, count, place)

    land_loads = []
    for block in range(flux_buf.shape[0]):
        lanes = pl.ds(block * cols, cols)
        land_loads.append(pltpu.make_async_copy(
            flux_ref.at[:, :, :, lanes], flux_buf.at[block], flux_sem.at[block]))
        land_loads.append(pltpu.make_async_copy(
            frac_ref.at[:, lanes], frac_buf.at[block], frac_sem.at[block]))
    for load in land_loads:
        load.start()
    order = [(offset, span) for span in first_spans for offset in flow_order(reach)]
    order += [(offset, span) for span in later_spans for offset in flow_order(reach)]
    order += [(reach, (0, slots))]
    loads = []
    for index, (offset, span) in enumerate(order):
        loads.append(pltpu.make_async_copy(
            weights_ref.at[offset, pl.ds(*span)], weights_buf.at[offset, pl.ds(*span)],
            weight_sem.at[index]))
    for load in loads[:EARLY]:
        load.start()

    lane = lax.broadcasted_iota(jnp.int32, (1, LANES), 1)
    mine = lax.rem(me, CLASSES)
    vote = jnp.where(lane <= CLASSES, 1, 0)
    for offset in range(num_off):
        live = count_ref[0, offset]
        if offset != reach:
            theirs = lax.rem(target(offset), CLASSES)
            fits = (lane == mine) | (lane == theirs) | (lane >= CLASSES) | (live <= half)
            vote = jnp.where(fits, vote, 0)
        vote = jnp.where(lane == COUNT_LANE + offset, live, vote)
    votes_ref[me] = vote

    for load in land_loads:
        load.wait()
    for load in loads[EARLY:]:
        load.start()

    def vote_copy(step):
        return pltpu.make_async_remote_copy(
            src_ref=votes_ref.at[me], dst_ref=votes_ref.at[me],
            send_sem=vote_send_sem.at[step], recv_sem=vote_recv_sem.at[step],
            device_id=place(lax.rem(me + step, count)), device_id_type=pl.DeviceIdType.MESH)

    def send_vote(step, carry):
        vote_copy(step).start()
        return carry

    def settle_vote(step, carry):
        source = lax.rem(me - step + count, count)
        pltpu.make_async_remote_copy(
            src_ref=votes_ref.at[me], dst_ref=votes_ref.at[source],
            send_sem=vote_send_sem.at[step], recv_sem=vote_recv_sem.at[step],
            device_id=place(source), device_id_type=pl.DeviceIdType.MESH).wait()
        return carry

    copies = []
    for index, (offset, span) in enumerate(order):
        begin, size = span
        loads[index].wait()

        def one_slot(slot, carry, offset=offset):
            block = col_ref[offset, 0, slot]
            frac = frac_buf[block]
            flux = flux_buf[block].astype(jnp.float32)
            flux = jnp.stack([flux[step] for step in range(num_steps)], axis=1)
            flux = flux.reshape(num_steps * num_kinds, tiles, cols)
            merged = jnp.sum(flux * frac[None], axis=1) / jnp.sum(frac, axis=0, keepdims=True)
            value = lax.dot_general(
                merged.astype(jnp.bfloat16), weights_buf[offset, slot],
                (((1,), (1,)), ((), ())), preferred_element_type=jnp.float32)
            if offset == reach:
                own_ref[slot] = value
            else:
                part_ref[offset, slot] = value
            return carry

        lax.fori_loop(begin, begin + size, one_slot, 0)
        if index == 0:
            pl.semaphore_wait(barrier, count - 1)
        if span in first_spans and offset != reach:
            chunk = first_spans.index(span)
            copy = pltpu.make_async_remote_copy(
                src_ref=part_ref.at[offset, pl.ds(begin, size)],
                dst_ref=arrived_ref.at[offset, pl.ds(begin, size)],
                send_sem=send_sem.at[offset, chunk], recv_sem=recv_sem.at[offset, chunk],
                device_id=place(target(offset)), device_id_type=pl.DeviceIdType.MESH)
            copy.start()
            copies.append(copy)
        if index == 0:
            lax.fori_loop(1, count, send_vote, 0)
        if begin == 0:
            if offset != reach:
                copy = pltpu.make_async_remote_copy(
                    src_ref=rows_ref.at[offset], dst_ref=arrived_rows_ref.at[offset],
                    send_sem=row_send_sem.at[offset], recv_sem=row_recv_sem.at[offset],
                    device_id=place(target(offset)), device_id_type=pl.DeviceIdType.MESH)
            else:
                copy = pltpu.make_async_copy(
                    rows_ref.at[reach], arrived_rows_ref.at[reach], own_sem)
            copy.start()
            copies.append(copy)
    lax.fori_loop(1, count, settle_vote, 0)
    agreed = jnp.min(votes_ref[:, 0, :], axis=0, keepdims=True)
    pick_ref[0] = jnp.min(jnp.where((agreed > 0) & (lane <= CLASSES), lane, CLASSES))
    for copy in copies:
        copy.wait()


def rest_kernel(axes, sizes, group, first, half, part_ref, arrived_ref, relay,
                base_send, base_recv, send_sem, recv_sem, pass_send, pass_recv,
                fwd_send, fwd_recv):
    num_off, slots = part_ref.shape[0], part_ref.shape[1]
    reach = num_off // 2
    outer, inner = sizes
    count = outer * inner
    x, y = lax.axis_index(axes[0]), lax.axis_index(axes[1])
    me = x * inner + y
    pieces = outer
    piece = (slots - half) // pieces

    def place(there):
        return (there // inner, lax.rem(there, inner))

    def shifted(device, offset):
        return lax.rem(device + offset - reach + count, count)

    def remote(src, dst, send, recv, device):
        return pltpu.make_async_remote_copy(
            src_ref=src, dst_ref=dst, send_sem=send, recv_sem=recv,
            device_id=device, device_id_type=pl.DeviceIdType.MESH)

    def hot(source, offset):
        goal = shifted(source, offset)
        return (lax.rem(source, CLASSES) == group) | (lax.rem(goal, CLASSES) == group)

    barrier = greet(me, count, place)
    pl.semaphore_wait(barrier, count - 1)

    def each_flow(act):
        def one(index, carry):
            away = reach - index // 2
            act(jnp.where(lax.rem(index, 2) == 0, reach + away, reach - away))
            return carry

        lax.fori_loop(0, 2 * reach, one, 0)

    def each_relay(act):
        def one(part, carry):
            source = lax.rem(x - part + outer, outer) * inner + y

            def flow(offset):
                @pl.when(hot(source, offset))
                def _():
                    act(offset, part, source)

            each_flow(flow)
            return carry

        lax.fori_loop(1, pieces, one, 0)

    ends = slots if group is None else half

    def base(offset):
        return remote(part_ref.at[offset, pl.ds(first, ends - first)],
                      arrived_ref.at[offset, pl.ds(0, ends - first)],
                      base_send.at[offset], base_recv.at[offset], place(shifted(me, offset)))

    if group is None:
        each_flow(lambda offset: base(offset).start())
        each_flow(lambda offset: base(offset).wait())
        return

    def direct(offset):
        return remote(part_ref.at[offset, pl.ds(half, piece)],
                      arrived_ref.at[offset, pl.ds(half - first, piece)],
                      send_sem.at[offset], recv_sem.at[offset], place(shifted(me, offset)))

    def detour(offset, part):
        return remote(part_ref.at[offset, pl.ds(half + part * piece, piece)],
                      relay.at[offset, part], pass_send.at[offset, part],
                      pass_recv.at[offset, part], (lax.rem(x + part, outer), y))

    def forward(offset, part, source):
        return remote(relay.at[offset, part],
                      arrived_ref.at[offset, pl.ds(half - first + part * piece, piece)],
                      fwd_send.at[offset, part], fwd_recv.at[offset, part],
                      place(shifted(source, offset)))

    def each_part(act):
        def one(part, carry):
            act(part)
            return carry

        lax.fori_loop(1, pieces, one, 0)

    def start_hot(offset):
        @pl.when(hot(me, offset))
        def _():
            each_part(lambda part: detour(offset, part).start())
            direct(offset).start()

    def pass_on(offset, part, source):
        detour(offset, part).wait_recv()
        forward(offset, part, source).start()

    def finish(offset):
        origin = lax.rem(me - offset + reach + count, count)

        @pl.when(hot(me, offset))
        def _():
            direct(offset).wait_send()
            each_part(lambda part: detour(offset, part).wait_send())

        @pl.when(hot(origin, offset))
        def _():
            direct(offset).wait_recv()
            each_part(lambda part: forward(offset, part, me).wait_recv())

        base(offset).wait()

    each_flow(start_hot)
    each_flow(lambda offset: base(offset).start())
    each_relay(pass_on)
    each_flow(finish)
    each_relay(lambda offset, part, source: forward(offset, part, source).wait_send())


def settle_kernel(axes, sizes, rows_ref, votes_ref, own_ref, low_ref, high_ref, out_ref,
                  rows, lives, total, out_buf, load_sem, live_sem, out_sem):
    num_off, first = low_ref.shape[0], low_ref.shape[1]
    reach = num_off // 2
    count = sizes[0] * sizes[1]
    me = lax.axis_index(axes[0]) * sizes[1] + lax.axis_index(axes[1])
    num_kinds, num_steps = out_ref.shape[0], out_ref.shape[1]
    blocks, _, block_rows = total.shape
    loads = [pltpu.make_async_copy(rows_ref, rows, load_sem)]
    for offset in range(num_off):
        source = lax.rem(me - offset + reach + count, count)
        loads.append(pltpu.make_async_copy(
            votes_ref.at[source], lives.at[offset], live_sem.at[offset]))
    for load in loads:
        load.start()
    total[...] = jnp.zeros_like(total)
    for load in loads:
        load.wait()
    for offset in range(num_off):
        live = lives[offset, 0, COUNT_LANE + offset]

        def add(slot, value, offset=offset):
            row = rows[offset, 0, slot]
            total[row] = total[row] + value

        def low_slot(slot, carry, offset=offset, add=add):
            add(slot, own_ref[slot] if offset == reach else low_ref[offset, slot])
            return carry

        def high_slot(slot, carry, offset=offset, add=add):
            add(slot, high_ref[offset, slot - first])
            return carry

        if offset == reach:
            lax.fori_loop(0, live, low_slot, 0)
        else:
            lax.fori_loop(0, jnp.minimum(live, first), low_slot, 0)
            lax.fori_loop(first, live, high_slot, 0)

    per_cut = blocks // OUT_CUTS
    stores = []
    for cut in range(OUT_CUTS):
        def one_block(block, carry):
            lanes = pl.ds(pl.multiple_of(block * block_rows, block_rows), block_rows)
            out_buf[:, :, lanes] = total[block].reshape(num_kinds, num_steps, block_rows)
            return carry

        lax.fori_loop(cut * per_cut, (cut + 1) * per_cut, one_block, 0, unroll=2)
        lanes = pl.ds(cut * per_cut * block_rows, per_cut * block_rows)
        store = pltpu.make_async_copy(
            out_buf.at[:, :, lanes], out_ref.at[:, :, lanes], out_sem.at[cut])
        store.start()
        stores.append(store)
    for store in stores:
        store.wait()


def on_device(axes, sizes, atm_blocks, tile_flux, tile_frac, weights, block_row, block_col,
              send_counts):
    num_steps, num_kinds = tile_flux.shape[0], tile_flux.shape[1]
    num_flux = num_steps * num_kinds
    num_off, slots, block_rows, block_cols = weights.shape[1:]
    tiles = tile_flux.shape[2]
    land_blocks = tile_flux.shape[3] // block_cols
    rows = block_row.transpose(1, 0, 2)
    columns = block_col.transpose(1, 0, 2)
    count = sizes[0] * sizes[1]
    half, first = slots // 2, slots // 4
    piece = (slots - half) // sizes[0]

    vmem = pl.BlockSpec(memory_space=pltpu.VMEM)
    smem = pl.BlockSpec(memory_space=pltpu.SMEM)
    hbm = pl.BlockSpec(memory_space=pltpu.HBM)
    dma = pltpu.SemaphoreType.DMA
    steps = 2 * slots * num_off
    part, own, low, arrived_rows, votes, pick = pl.pallas_call(
        functools.partial(exchange_kernel, axes, sizes, first, half),
        out_shape=(
            pltpu.VMEM((num_off, slots, num_flux, block_rows), jnp.float32),
            pltpu.VMEM((slots, num_flux, block_rows), jnp.float32),
            pltpu.VMEM((num_off, first, num_flux, block_rows), jnp.float32),
            pltpu.VMEM(rows.shape, jnp.int32),
            pltpu.VMEM((count, 1, LANES), jnp.int32),
            jax.ShapeDtypeStruct((1,), jnp.int32),
        ),
        in_specs=[hbm, hbm, smem, smem, hbm, hbm],
        out_specs=(vmem, vmem, vmem, vmem, vmem, smem),
        scratch_shapes=[
            pltpu.VMEM((land_blocks, num_steps, num_kinds, tiles, block_cols), tile_flux.dtype),
            pltpu.VMEM((land_blocks, tiles, block_cols), tile_frac.dtype),
            pltpu.VMEM(weights.shape[1:], weights.dtype),
            dma((land_blocks,)),
            dma((land_blocks,)),
            dma((steps,)),
            dma,
            dma((num_off, first)),
            dma((num_off, first)),
            dma((num_off,)),
            dma((num_off,)),
            dma((count,)),
            dma((count,)),
        ],
        compiler_params=pltpu.CompilerParams(collective_id=0, has_side_effects=True,
                                             vmem_limit_bytes=55 * 2**20),
        name="exchange",
    )(tile_flux, tile_frac, columns, send_counts, rows, weights[0])

    def settle(arrived_rows, votes, own, low, high):
        return pl.pallas_call(
            functools.partial(settle_kernel, axes, sizes),
            out_shape=jax.ShapeDtypeStruct((num_kinds, num_steps, atm_blocks * block_rows),
                                           jnp.float32),
            in_specs=[vmem] * 5,
            out_specs=hbm,
            scratch_shapes=[
                pltpu.SMEM(rows.shape, jnp.int32),
                pltpu.SMEM((num_off, 1, LANES), jnp.int32),
                pltpu.VMEM((atm_blocks, num_flux, block_rows), jnp.float32),
                pltpu.VMEM((num_kinds, num_steps, atm_blocks * block_rows), jnp.float32),
                dma,
                dma((num_off,)),
                dma((OUT_CUTS,)),
            ],
            compiler_params=pltpu.CompilerParams(vmem_limit_bytes=16 * 2**20),
            name="settle",
        )(arrived_rows, votes, own, low, high)

    def rest(group):
        def call(part, arrived_rows, votes, own, low):
            high = pl.pallas_call(
                functools.partial(rest_kernel, axes, sizes, group, first, half),
                out_shape=pltpu.VMEM((num_off, slots - first, num_flux, block_rows),
                                     jnp.float32),
                in_specs=[vmem],
                out_specs=vmem,
                scratch_shapes=[
                    pltpu.VMEM((num_off, sizes[0], piece, num_flux, block_rows), jnp.float32),
                ] + [dma((num_off,))] * 4 + [dma((num_off, sizes[0]))] * 4,
                compiler_params=pltpu.CompilerParams(
                    collective_id=CLASSES + 1 if group is None else 1 + group,
                    has_side_effects=True, vmem_limit_bytes=16 * 2**20),
                name="rest",
            )(part)
            return settle(arrived_rows, votes, own, low, high)
        return call

    groups = list(range(CLASSES)) + [None]
    out = lax.switch(pick[0], [rest(group) for group in groups],
                     part, arrived_rows, votes, own, low)
    return out.transpose(1, 0, 2)


def solution(mesh):
    axes = ("gx", "gy")
    sizes = (mesh.shape["gx"], mesh.shape["gy"])
    return jax.shard_map(
        functools.partial(on_device, axes, sizes, AB_DEV),
        mesh=mesh,
        in_specs=(
            P(None, None, None, ("gx", "gy")),
            P(None, ("gx", "gy")),
            P(("gx", "gy"), None, None, None, None),
            P(("gx", "gy"), None, None),
            P(("gx", "gy"), None, None),
            P(("gx", "gy"), None),
        ),
        out_specs=P(None, None, ("gx", "gy")),
        check_vma=False,
    )
```

```python
import functools

import jax
import jax.numpy as jnp
from jax import lax
from jax.experimental import pallas as pl
from jax.experimental.pallas import tpu as pltpu
from jax.sharding import PartitionSpec as P

OUT_CUTS = 4
EARLY = 4
MAX_CLASSES = 32
CORES = 2
LANES = 128
AB_DEV = 48


def ranges(begin, end, sizes):
    spans = []
    for size in sizes:
        size = min(size, end - begin)
        if size > 0:
            spans.append((begin, size))
            begin += size
    if begin < end:
        spans.append((begin, end - begin))
    return spans


def flow_order(reach):
    order = []
    for away in range(reach, 0, -1):
        order += [reach + away, reach - away]
    return order


def flip(index, bits):
    out, weight = index, 1
    while weight <= bits:
        if bits // weight % 2:
            out = out + weight - 2 * weight * lax.rem(index // weight, 2)
        weight *= 2
    return out


def exchange_kernel(axes, sizes, classes, first, half, flux_ref, frac_ref, col_ref, count_ref, rows_ref,
                    weights_ref, part_ref, own_ref, arrived_ref, arrived_meta_ref, pick_ref,
                    flux_buf, frac_buf, weights_buf, meta, column_votes, row_votes,
                    flux_sem, frac_sem, weight_sem, meta_sem, own_sem, send_sem, recv_sem,
                    meta_send_sem, meta_recv_sem, column_send_sem, column_recv_sem,
                    row_send_sem, row_recv_sem):
    num_off, slots = weights_buf.shape[0], weights_buf.shape[1]
    num_steps, num_kinds, tiles, _ = flux_ref.shape
    cols = weights_buf.shape[3]
    reach = num_off // 2
    outer, inner = sizes
    count = outer * inner
    x, y = lax.axis_index(axes[0]), lax.axis_index(axes[1])
    me = x * inner + y
    first_spans = ranges(0, first, (1, 1, 2))
    later_spans = ranges(first, slots, (half - first,))

    def place(there):
        return (there // inner, lax.rem(there, inner))

    def target(offset):
        return lax.rem(me + offset - reach + count, count)

    def steps(size, act):
        def one(step, carry):
            act(step)
            return carry

        lax.fori_loop(1, size, one, 0)

    barrier = pltpu.get_barrier_semaphore()
    greeted = 2 * reach + outer - 1 + inner - 1

    def greet(device):
        pl.semaphore_signal(barrier, inc=1, device_id=device,
                            device_id_type=pl.DeviceIdType.MESH)

    for offset in flow_order(reach):
        greet(place(target(offset)))
    steps(outer, lambda step: greet((lax.rem(x + step, outer), y)))
    steps(inner, lambda step: greet((x, lax.rem(y + step, inner))))

    land_loads = []
    for block in range(flux_buf.shape[0]):
        lanes = pl.ds(block * cols, cols)
        land_loads.append(pltpu.make_async_copy(
            flux_ref.at[:, :, :, lanes], flux_buf.at[block], flux_sem.at[block]))
        land_loads.append(pltpu.make_async_copy(
            frac_ref.at[:, lanes], frac_buf.at[block], frac_sem.at[block]))
    for load in land_loads:
        load.start()
    meta_loads = [pltpu.make_async_copy(rows_ref.at[offset], meta.at[offset, 0],
                                        meta_sem.at[offset]) for offset in range(num_off)]
    for load in meta_loads:
        load.start()
    order = [(offset, span) for span in first_spans for offset in flow_order(reach)]
    order += [(offset, span) for span in later_spans for offset in flow_order(reach)]
    order += [(reach, (0, slots))]
    loads = []
    for index, (offset, span) in enumerate(order):
        loads.append(pltpu.make_async_copy(
            weights_ref.at[offset, pl.ds(*span)], weights_buf.at[offset, pl.ds(*span)],
            weight_sem.at[index]))
    for load in loads[:EARLY]:
        load.start()

    lane = lax.broadcasted_iota(jnp.int32, (1, LANES), 1)
    mine = lax.rem(me, classes)
    vote = jnp.where(lane <= classes, 1, 0)
    for offset in range(num_off):
        live = count_ref[0, offset]
        meta[offset, 1] = jnp.full((1, slots), live, jnp.int32)
        if offset != reach:
            theirs = lax.rem(target(offset), classes)
            fits = (lane == mine) | (lane == theirs) | (lane >= classes) | (live <= half)
            vote = jnp.where(fits, vote, 0)
    column_votes[x] = vote

    for load in land_loads:
        load.wait()
    for load in loads[EARLY:]:
        load.start()

    def column_vote(step, source):
        return pltpu.make_async_remote_copy(
            src_ref=column_votes.at[x], dst_ref=column_votes.at[source],
            send_sem=column_send_sem.at[step], recv_sem=column_recv_sem.at[step],
            device_id=(lax.rem(x + step, outer), y), device_id_type=pl.DeviceIdType.MESH)

    def row_vote(step, source):
        return pltpu.make_async_remote_copy(
            src_ref=row_votes.at[y], dst_ref=row_votes.at[source],
            send_sem=row_send_sem.at[step], recv_sem=row_recv_sem.at[step],
            device_id=(x, lax.rem(y + step, inner)), device_id_type=pl.DeviceIdType.MESH)

    copies = []
    for index, (offset, span) in enumerate(order):
        begin, size = span
        loads[index].wait()

        def one_slot(slot, carry, offset=offset):
            block = col_ref[offset, 0, slot]
            frac = frac_buf[block]
            flux = flux_buf[block].astype(jnp.float32)
            flux = jnp.stack([flux[step] for step in range(num_steps)], axis=1)
            flux = flux.reshape(num_steps * num_kinds, tiles, cols)
            merged = jnp.sum(flux * frac[None], axis=1) / jnp.sum(frac, axis=0, keepdims=True)
            value = lax.dot_general(
                merged.astype(jnp.bfloat16), weights_buf[offset, slot],
                (((1,), (1,)), ((), ())), preferred_element_type=jnp.float32)
            if offset == reach:
                own_ref[slot] = value
            else:
                part_ref[offset, slot] = value
            return carry

        lax.fori_loop(begin, begin + size, one_slot, 0, unroll=2 if size % 2 == 0 else 1)
        if index == 0:
            pl.semaphore_wait(barrier, greeted)
        if span in first_spans and offset != reach:
            chunk = first_spans.index(span)
            copy = pltpu.make_async_remote_copy(
                src_ref=part_ref.at[offset, pl.ds(begin, size)],
                dst_ref=arrived_ref.at[offset, pl.ds(begin, size)],
                send_sem=send_sem.at[offset, chunk], recv_sem=recv_sem.at[offset, chunk],
                device_id=place(target(offset)), device_id_type=pl.DeviceIdType.MESH)
            copy.start()
            copies.append(copy)
        if index == 0:
            steps(outer, lambda step: column_vote(step, x).start())
            for load in meta_loads:
                load.wait()
        if begin == 0:
            if offset != reach:
                copy = pltpu.make_async_remote_copy(
                    src_ref=meta.at[offset], dst_ref=arrived_meta_ref.at[offset],
                    send_sem=meta_send_sem.at[offset], recv_sem=meta_recv_sem.at[offset],
                    device_id=place(target(offset)), device_id_type=pl.DeviceIdType.MESH)
            else:
                copy = pltpu.make_async_copy(
                    meta.at[reach], arrived_meta_ref.at[reach], own_sem)
            copy.start()
            copies.append(copy)
        if index == 4 * reach - 1:
            steps(outer, lambda step: column_vote(
                step, lax.rem(x - step + outer, outer)).wait())
            row_votes[y] = jnp.min(column_votes[:, 0, :], axis=0, keepdims=True)
            steps(inner, lambda step: row_vote(step, y).start())
    steps(inner, lambda step: row_vote(step, lax.rem(y - step + inner, inner)).wait())
    agreed = jnp.min(row_votes[:, 0, :], axis=0, keepdims=True)
    pick_ref[0] = jnp.min(jnp.where((agreed > 0) & (lane <= classes), lane, classes))
    for copy in copies:
        copy.wait()


def rest_kernel(axes, sizes, classes, group, first, half, detours, part_ref, arrived_ref, relay,
                early_send, early_recv, late_send, late_recv, send_sem, recv_sem,
                pass_send, pass_recv, fwd_send, fwd_recv):
    num_off, slots = part_ref.shape[0], part_ref.shape[1]
    reach = num_off // 2
    outer, inner = sizes
    count = outer * inner
    x, y = lax.axis_index(axes[0]), lax.axis_index(axes[1])
    me = x * inner + y
    middle = (first + half) // 2
    straight = slots - half - sum(size for _, size in detours)

    def place(there):
        return (there // inner, lax.rem(there, inner))

    def shifted(device, offset):
        return lax.rem(device + offset - reach + count, count)

    def origin(offset):
        return lax.rem(me - offset + reach + count, count)

    def remote(src, dst, send, recv, device):
        return pltpu.make_async_remote_copy(
            src_ref=src, dst_ref=dst, send_sem=send, recv_sem=recv,
            device_id=device, device_id_type=pl.DeviceIdType.MESH)

    def heavy(source, offset):
        goal = shifted(source, offset)
        return (lax.rem(source, classes) == group) | (lax.rem(goal, classes) == group)

    def near(source, offset):
        return source // CORES == shifted(source, offset) // CORES

    def hot(source, offset):
        return heavy(source, offset) & jnp.logical_not(near(source, offset))

    def close(source, offset):
        return heavy(source, offset) & near(source, offset)

    def each_flow(act):
        def one(index, carry):
            away = reach - index // 2
            act(jnp.where(lax.rem(index, 2) == 0, reach + away, reach - away))
            return carry

        lax.fori_loop(0, 2 * reach, one, 0)

    def span(offset, begin, end, send, recv):
        return remote(part_ref.at[offset, pl.ds(begin, end - begin)],
                      arrived_ref.at[offset, pl.ds(begin - first, end - begin)],
                      send.at[offset], recv.at[offset], place(shifted(me, offset)))

    def early(offset):
        return span(offset, first, slots if group is None else middle, early_send, early_recv)

    def late(offset):
        return span(offset, middle, half, late_send, late_recv)

    def direct(offset):
        return span(offset, half, half + straight, send_sem, recv_sem)

    def whole(offset):
        return span(offset, half, slots, send_sem, recv_sem)

    barrier = pltpu.get_barrier_semaphore()

    def greet(device):
        pl.semaphore_signal(barrier, inc=1, device_id=device,
                            device_id_type=pl.DeviceIdType.MESH)

    each_flow(lambda offset: greet(place(shifted(me, offset))))
    if group is None:
        pl.semaphore_wait(barrier, 2 * reach)
        each_flow(lambda offset: early(offset).start())
        each_flow(lambda offset: early(offset).wait())
        return

    routes, begin = [], half + straight
    for index, (bits, size) in enumerate(detours):
        routes.append((index, bits, begin, size))
        begin += size

    def detour(offset, route):
        index, bits, begin, size = route
        return remote(part_ref.at[offset, pl.ds(begin, size)],
                      relay.at[offset, pl.ds(begin - half, size)], pass_send.at[offset, index],
                      pass_recv.at[offset, index], (flip(x, bits), y))

    def forward(offset, route, source):
        index, bits, begin, size = route
        return remote(relay.at[offset, pl.ds(begin - half, size)],
                      arrived_ref.at[offset, pl.ds(begin - first, size)],
                      fwd_send.at[offset, index], fwd_recv.at[offset, index],
                      place(shifted(source, offset)))

    def greet_route(offset, total):
        here, there = hot(me, offset), hot(origin(offset), offset)
        for _, bits, _, _ in routes:
            source = flip(x, bits) * inner + y
            middleman = hot(source, offset)

            @pl.when(here | middleman)
            def _():
                greet((flip(x, bits), y))

            @pl.when(middleman)
            def _():
                greet(place(shifted(source, offset)))

            @pl.when(there)
            def _():
                begun = origin(offset)
                greet((flip(begun // inner, bits), lax.rem(begun, inner)))

            total = (total + jnp.where(here | middleman, 1, 0) + jnp.where(middleman, 1, 0)
                     + jnp.where(there, 1, 0))
        return total

    def greet_one(index, total):
        away = reach - index // 2
        return greet_route(jnp.where(lax.rem(index, 2) == 0, reach + away, reach - away), total)

    pl.semaphore_wait(barrier, lax.fori_loop(0, 2 * reach, greet_one, 2 * reach))

    def start_hot(offset):
        @pl.when(hot(me, offset))
        def _():
            for route in routes:
                detour(offset, route).start()
            direct(offset).start()

        @pl.when(close(me, offset))
        def _():
            whole(offset).start()

    def pass_on(offset):
        for route in routes:
            source = flip(x, route[1]) * inner + y

            @pl.when(hot(source, offset))
            def _(route=route, source=source):
                detour(offset, route).wait_recv()
                forward(offset, route, source).start()

    def finish(offset):
        early(offset).wait()
        late(offset).wait()

        @pl.when(close(me, offset))
        def _():
            whole(offset).wait_send()

        @pl.when(close(origin(offset), offset))
        def _():
            whole(offset).wait_recv()

        @pl.when(hot(me, offset))
        def _():
            direct(offset).wait_send()
            for route in routes:
                detour(offset, route).wait_send()

        @pl.when(hot(origin(offset), offset))
        def _():
            direct(offset).wait_recv()
            for route in routes:
                forward(offset, route, me).wait_recv()

        for route in routes:
            source = flip(x, route[1]) * inner + y

            @pl.when(hot(source, offset))
            def _(route=route, source=source):
                forward(offset, route, source).wait_send()

    each_flow(start_hot)
    each_flow(lambda offset: early(offset).start())
    each_flow(pass_on)
    each_flow(lambda offset: late(offset).start())
    each_flow(finish)


def settle_kernel(meta_ref, own_ref, low_ref, high_ref, out_ref, meta, total, out_buf,
                  load_sem, out_sem):
    num_off, first = low_ref.shape[0], low_ref.shape[1]
    reach = num_off // 2
    num_kinds, num_steps = out_ref.shape[0], out_ref.shape[1]
    blocks, _, block_rows = total.shape
    load = pltpu.make_async_copy(meta_ref, meta, load_sem)
    load.start()

    def clear(block, carry):
        total[block] = jnp.zeros_like(total[block])
        return carry

    lax.fori_loop(0, blocks, clear, 0, unroll=4)
    load.wait()

    def add(offset, slot, value):
        row = meta[offset, 0, 0, slot]
        total[row] = total[row] + value

    def one_flow(offset, carry):
        live = meta[offset, 1, 0, 0]

        def low_slot(slot, carry):
            add(offset, slot, low_ref[offset, slot])
            return carry

        def high_slot(slot, carry):
            add(offset, slot, high_ref[offset, slot - first])
            return carry

        @pl.when(offset != reach)
        def _():
            lax.fori_loop(0, jnp.minimum(live, first), low_slot, 0)
            lax.fori_loop(first, live, high_slot, 0)

        return carry

    def own_slot(slot, carry):
        add(reach, slot, own_ref[slot])
        return carry

    lax.fori_loop(0, num_off, one_flow, 0)
    lax.fori_loop(0, meta[reach, 1, 0, 0], own_slot, 0)

    per_cut = blocks // OUT_CUTS
    stores = []
    for cut in range(OUT_CUTS):
        def one_block(block, carry):
            lanes = pl.ds(pl.multiple_of(block * block_rows, block_rows), block_rows)
            out_buf[:, :, lanes] = total[block].reshape(num_kinds, num_steps, block_rows)
            return carry

        lax.fori_loop(cut * per_cut, (cut + 1) * per_cut, one_block, 0, unroll=2)
        lanes = pl.ds(cut * per_cut * block_rows, per_cut * block_rows)
        store = pltpu.make_async_copy(
            out_buf.at[:, :, lanes], out_ref.at[:, :, lanes], out_sem.at[cut])
        store.start()
        stores.append(store)
    for store in stores:
        store.wait()


def on_device(axes, sizes, atm_blocks, tile_flux, tile_frac, weights, block_row, block_col,
              send_counts):
    num_steps, num_kinds = tile_flux.shape[0], tile_flux.shape[1]
    num_flux = num_steps * num_kinds
    num_off, slots, block_rows, block_cols = weights.shape[1:]
    tiles = tile_flux.shape[2]
    land_blocks = tile_flux.shape[3] // block_cols
    rows = block_row.transpose(1, 0, 2)
    columns = block_col.transpose(1, 0, 2)
    count = sizes[0] * sizes[1]
    half, first = slots // 2, slots // 4
    share = (slots - half) // 8
    detours = ((1, 2 * share), (2, 3 * share)) if sizes[0] % 4 == 0 else ()
    classes = min(count, MAX_CLASSES)

    vmem = pl.BlockSpec(memory_space=pltpu.VMEM)
    smem = pl.BlockSpec(memory_space=pltpu.SMEM)
    hbm = pl.BlockSpec(memory_space=pltpu.HBM)
    dma = pltpu.SemaphoreType.DMA
    steps = 2 * slots * num_off
    part, own, low, arrived_meta, pick = pl.pallas_call(
        functools.partial(exchange_kernel, axes, sizes, classes, first, half),
        out_shape=(
            pltpu.VMEM((num_off, slots, num_flux, block_rows), jnp.float32),
            pltpu.VMEM((slots, num_flux, block_rows), jnp.float32),
            pltpu.VMEM((num_off, first, num_flux, block_rows), jnp.float32),
            pltpu.VMEM((num_off, 2, 1, slots), jnp.int32),
            jax.ShapeDtypeStruct((1,), jnp.int32),
        ),
        in_specs=[hbm, hbm, smem, smem, hbm, hbm],
        out_specs=(vmem, vmem, vmem, vmem, smem),
        scratch_shapes=[
            pltpu.VMEM((land_blocks, num_steps, num_kinds, tiles, block_cols), tile_flux.dtype),
            pltpu.VMEM((land_blocks, tiles, block_cols), tile_frac.dtype),
            pltpu.VMEM(weights.shape[1:], weights.dtype),
            pltpu.VMEM((num_off, 2, 1, slots), jnp.int32),
            pltpu.VMEM((sizes[0], 1, LANES), jnp.int32),
            pltpu.VMEM((sizes[1], 1, LANES), jnp.int32),
            dma((land_blocks,)),
            dma((land_blocks,)),
            dma((steps,)),
            dma((num_off,)),
            dma,
            dma((num_off, first)),
            dma((num_off, first)),
            dma((num_off,)),
            dma((num_off,)),
            dma((sizes[0],)),
            dma((sizes[0],)),
            dma((sizes[1],)),
            dma((sizes[1],)),
        ],
        compiler_params=pltpu.CompilerParams(collective_id=0, has_side_effects=True,
                                             vmem_limit_bytes=55 * 2**20),
        name="exchange",
    )(tile_flux, tile_frac, columns, send_counts, rows, weights[0])

    def settle(arrived_meta, own, low, high):
        return pl.pallas_call(
            settle_kernel,
            out_shape=jax.ShapeDtypeStruct((num_kinds, num_steps, atm_blocks * block_rows),
                                           jnp.float32),
            in_specs=[vmem] * 4,
            out_specs=hbm,
            scratch_shapes=[
                pltpu.SMEM((num_off, 2, 1, slots), jnp.int32),
                pltpu.VMEM((atm_blocks, num_flux, block_rows), jnp.float32),
                pltpu.VMEM((num_kinds, num_steps, atm_blocks * block_rows), jnp.float32),
                dma,
                dma((OUT_CUTS,)),
            ],
            compiler_params=pltpu.CompilerParams(vmem_limit_bytes=16 * 2**20),
            name="settle",
        )(arrived_meta, own, low, high)

    def rest(group):
        def call(part, arrived_meta, own, low):
            high = pl.pallas_call(
                functools.partial(rest_kernel, axes, sizes, classes, group, first, half, detours),
                out_shape=pltpu.VMEM((num_off, slots - first, num_flux, block_rows),
                                     jnp.float32),
                in_specs=[vmem],
                out_specs=vmem,
                scratch_shapes=[
                    pltpu.VMEM((num_off, slots - half, num_flux, block_rows), jnp.float32),
                ] + [dma((num_off,))] * 6 + [dma((num_off, max(len(detours), 1)))] * 4,
                compiler_params=pltpu.CompilerParams(
                    collective_id=classes + 1 if group is None else 1 + group,
                    has_side_effects=True, vmem_limit_bytes=16 * 2**20),
                name="rest",
            )(part)
            return settle(arrived_meta, own, low, high)
        return call

    groups = list(range(classes)) + [None]
    out = lax.switch(pick[0], [rest(group) for group in groups],
                     part, arrived_meta, own, low)
    return out.transpose(1, 0, 2)


def solution(mesh):
    axes = ("gx", "gy")
    sizes = (mesh.shape["gx"], mesh.shape["gy"])
    return jax.shard_map(
        functools.partial(on_device, axes, sizes, AB_DEV),
        mesh=mesh,
        in_specs=(
            P(None, None, None, ("gx", "gy")),
            P(None, ("gx", "gy")),
            P(("gx", "gy"), None, None, None, None),
            P(("gx", "gy"), None, None),
            P(("gx", "gy"), None, None),
            P(("gx", "gy"), None),
        ),
        out_specs=P(None, None, ("gx", "gy")),
        check_vma=False,
    )
```

```python
import functools

import jax
import jax.numpy as jnp
from jax import lax
from jax.experimental import pallas as pl
from jax.experimental.pallas import tpu as pltpu
from jax.sharding import PartitionSpec as P

OUT_CUTS = 4
EARLY = 4
MAX_CLASSES = 32
CORES = 2
LANES = 128
AB_DEV = 48


def ranges(begin, end, sizes):
    spans = []
    for size in sizes:
        size = min(size, end - begin)
        if size > 0:
            spans.append((begin, size))
            begin += size
    if begin < end:
        spans.append((begin, end - begin))
    return spans


def flow_order(reach):
    order = []
    for away in range(reach, 0, -1):
        order += [reach + away, reach - away]
    return order


def flip(index, bits, size):
    out, weight = index, 1
    while weight < size:
        mine, theirs = lax.rem(index // weight, 2), lax.rem(bits // weight, 2)
        out = out + weight * theirs * (1 - 2 * mine)
        weight *= 2
    return out


def exchange_kernel(axes, sizes, classes, first, half, flux_ref, frac_ref, col_ref, count_ref, rows_ref,
                    weights_ref, part_ref, own_ref, arrived_ref, arrived_meta_ref, pick_ref,
                    flux_buf, frac_buf, weights_buf, meta, column_votes, row_votes,
                    flux_sem, frac_sem, weight_sem, meta_sem, own_sem, send_sem, recv_sem,
                    meta_send_sem, meta_recv_sem, column_send_sem, column_recv_sem,
                    row_send_sem, row_recv_sem):
    num_off, slots = weights_buf.shape[0], weights_buf.shape[1]
    num_steps, num_kinds, tiles, _ = flux_ref.shape
    cols = weights_buf.shape[3]
    reach = num_off // 2
    outer, inner = sizes
    count = outer * inner
    x, y = lax.axis_index(axes[0]), lax.axis_index(axes[1])
    me = x * inner + y
    first_spans = ranges(0, first, (1, 1, 2))
    later_spans = ranges(first, slots, (half - first,))

    def place(there):
        return (there // inner, lax.rem(there, inner))

    def target(offset):
        return lax.rem(me + offset - reach + count, count)

    def steps(size, act):
        def one(step, carry):
            act(step)
            return carry

        lax.fori_loop(1, size, one, 0)

    barrier = pltpu.get_barrier_semaphore()
    greeted = 2 * reach + outer - 1 + inner - 1

    def greet(device):
        pl.semaphore_signal(barrier, inc=1, device_id=device,
                            device_id_type=pl.DeviceIdType.MESH)

    for offset in flow_order(reach):
        greet(place(target(offset)))
    steps(outer, lambda step: greet((lax.rem(x + step, outer), y)))
    steps(inner, lambda step: greet((x, lax.rem(y + step, inner))))

    land_loads = []
    for block in range(flux_buf.shape[0]):
        lanes = pl.ds(block * cols, cols)
        land_loads.append(pltpu.make_async_copy(
            flux_ref.at[:, :, :, lanes], flux_buf.at[block], flux_sem.at[block]))
        land_loads.append(pltpu.make_async_copy(
            frac_ref.at[:, lanes], frac_buf.at[block], frac_sem.at[block]))
    for load in land_loads:
        load.start()
    meta_loads = [pltpu.make_async_copy(rows_ref.at[offset], meta.at[offset, 0],
                                        meta_sem.at[offset]) for offset in range(num_off)]
    for load in meta_loads:
        load.start()
    order = [(offset, span) for span in first_spans for offset in flow_order(reach)]
    order += [(offset, span) for span in later_spans for offset in flow_order(reach)]
    order += [(reach, (0, slots))]
    loads = []
    for index, (offset, span) in enumerate(order):
        loads.append(pltpu.make_async_copy(
            weights_ref.at[offset, pl.ds(*span)], weights_buf.at[offset, pl.ds(*span)],
            weight_sem.at[index]))
    for load in loads[:EARLY]:
        load.start()

    lane = lax.broadcasted_iota(jnp.int32, (1, LANES), 1)
    mine = lax.rem(me, classes)
    vote = jnp.where(lane <= classes, 1, 0)
    for offset in range(num_off):
        live = count_ref[0, offset]
        meta[offset, 1] = jnp.full((1, slots), live, jnp.int32)
        if offset != reach:
            theirs = lax.rem(target(offset), classes)
            fits = (lane == mine) | (lane == theirs) | (lane >= classes) | (live <= half)
            vote = jnp.where(fits, vote, 0)
    column_votes[x] = vote

    for load in land_loads:
        load.wait()
    for load in loads[EARLY:]:
        load.start()

    def column_vote(step, source):
        return pltpu.make_async_remote_copy(
            src_ref=column_votes.at[x], dst_ref=column_votes.at[source],
            send_sem=column_send_sem.at[step], recv_sem=column_recv_sem.at[step],
            device_id=(lax.rem(x + step, outer), y), device_id_type=pl.DeviceIdType.MESH)

    def row_vote(step, source):
        return pltpu.make_async_remote_copy(
            src_ref=row_votes.at[y], dst_ref=row_votes.at[source],
            send_sem=row_send_sem.at[step], recv_sem=row_recv_sem.at[step],
            device_id=(x, lax.rem(y + step, inner)), device_id_type=pl.DeviceIdType.MESH)

    copies = []
    for index, (offset, span) in enumerate(order):
        begin, size = span
        loads[index].wait()

        def one_slot(slot, carry, offset=offset):
            block = col_ref[offset, 0, slot]
            frac = frac_buf[block]
            flux = flux_buf[block].astype(jnp.float32)
            flux = jnp.stack([flux[step] for step in range(num_steps)], axis=1)
            flux = flux.reshape(num_steps * num_kinds, tiles, cols)
            merged = jnp.sum(flux * frac[None], axis=1) / jnp.sum(frac, axis=0, keepdims=True)
            value = lax.dot_general(
                merged.astype(jnp.bfloat16), weights_buf[offset, slot],
                (((1,), (1,)), ((), ())), preferred_element_type=jnp.float32)
            if offset == reach:
                own_ref[slot] = value
            else:
                part_ref[offset, slot] = value
            return carry

        lax.fori_loop(begin, begin + size, one_slot, 0, unroll=2 if size % 2 == 0 else 1)
        if index == 0:
            pl.semaphore_wait(barrier, greeted)
        if span in first_spans and offset != reach:
            chunk = first_spans.index(span)
            copy = pltpu.make_async_remote_copy(
                src_ref=part_ref.at[offset, pl.ds(begin, size)],
                dst_ref=arrived_ref.at[offset, pl.ds(begin, size)],
                send_sem=send_sem.at[offset, chunk], recv_sem=recv_sem.at[offset, chunk],
                device_id=place(target(offset)), device_id_type=pl.DeviceIdType.MESH)
            copy.start()
            copies.append(copy)
        if index == 0:
            steps(outer, lambda step: column_vote(step, x).start())
            for load in meta_loads:
                load.wait()
        if begin == 0:
            if offset != reach:
                copy = pltpu.make_async_remote_copy(
                    src_ref=meta.at[offset], dst_ref=arrived_meta_ref.at[offset],
                    send_sem=meta_send_sem.at[offset], recv_sem=meta_recv_sem.at[offset],
                    device_id=place(target(offset)), device_id_type=pl.DeviceIdType.MESH)
            else:
                copy = pltpu.make_async_copy(
                    meta.at[reach], arrived_meta_ref.at[reach], own_sem)
            copy.start()
            copies.append(copy)
        if index == 4 * reach - 1:
            steps(outer, lambda step: column_vote(
                step, lax.rem(x - step + outer, outer)).wait())
            row_votes[y] = jnp.min(column_votes[:, 0, :], axis=0, keepdims=True)
            steps(inner, lambda step: row_vote(step, y).start())
    steps(inner, lambda step: row_vote(step, lax.rem(y - step + inner, inner)).wait())
    agreed = jnp.min(row_votes[:, 0, :], axis=0, keepdims=True)
    pick_ref[0] = jnp.min(jnp.where((agreed > 0) & (lane <= classes), lane, classes))
    for copy in copies:
        copy.wait()


def rest_kernel(axes, sizes, classes, group, first, half, parts, part_ref, arrived_ref, relay,
                base_send, base_recv, send_sem, recv_sem, pass_send, pass_recv,
                fwd_send, fwd_recv):
    num_off, slots = part_ref.shape[0], part_ref.shape[1]
    reach = num_off // 2
    outer, inner = sizes
    count = outer * inner
    x, y = lax.axis_index(axes[0]), lax.axis_index(axes[1])
    me = x * inner + y
    batch = (half - first) // 2
    piece = (slots - half) // parts

    def place(there):
        return (there // inner, lax.rem(there, inner))

    def shifted(device, offset):
        return lax.rem(device + offset - reach + count, count)

    def origin(offset):
        return lax.rem(me - offset + reach + count, count)

    def beside(part):
        return flip(x, part, outer)

    def remote(src, dst, send, recv, device):
        return pltpu.make_async_remote_copy(
            src_ref=src, dst_ref=dst, send_sem=send, recv_sem=recv,
            device_id=device, device_id_type=pl.DeviceIdType.MESH)

    def member(device):
        return (device if classes == count else lax.rem(device, classes)) == group

    def heavy(source, goal):
        return member(source) | member(goal)

    def near(source, goal):
        return source // CORES == goal // CORES

    def hot(source, offset):
        goal = shifted(source, offset)
        return heavy(source, goal) & jnp.logical_not(near(source, goal))

    def close(source, offset):
        goal = shifted(source, offset)
        return heavy(source, goal) & near(source, goal)

    def repeat(begin, end, act):
        def one(step, carry):
            act(step)
            return carry

        lax.fori_loop(begin, end, one, 0)

    def each_flow(act):
        def one(index):
            away = reach - index // 2
            act(jnp.where(lax.rem(index, 2) == 0, reach + away, reach - away))

        repeat(0, 2 * reach, one)

    def each_part(act):
        repeat(1, parts, act)

    def span(offset, begin, size, send, recv):
        return remote(part_ref.at[offset, pl.ds(begin, size)],
                      arrived_ref.at[offset, pl.ds(begin - first, size)],
                      send, recv, place(shifted(me, offset)))

    def base(offset, step):
        size = slots - first if group is None else batch
        return span(offset, first + step * batch, size, base_send.at[offset, step],
                    base_recv.at[offset, step])

    def direct(offset):
        return span(offset, half, piece, send_sem.at[offset], recv_sem.at[offset])

    def whole(offset):
        return span(offset, half, slots - half, send_sem.at[offset], recv_sem.at[offset])

    def detour(offset, part):
        return remote(part_ref.at[offset, pl.ds(half + part * piece, piece)],
                      relay.at[offset, part], pass_send.at[offset, part],
                      pass_recv.at[offset, part], (beside(part), y))

    def forward(offset, part, source):
        return remote(relay.at[offset, part],
                      arrived_ref.at[offset, pl.ds(half - first + part * piece, piece)],
                      fwd_send.at[offset, part], fwd_recv.at[offset, part],
                      place(shifted(source, offset)))

    barrier = pltpu.get_barrier_semaphore()

    def greet(device, inc=1):
        pl.semaphore_signal(barrier, inc=inc, device_id=device,
                            device_id_type=pl.DeviceIdType.MESH)

    each_flow(lambda offset: greet(place(shifted(me, offset))))
    if group is None:
        pl.semaphore_wait(barrier, 2 * reach)
        each_flow(lambda offset: base(offset, 0).start())
        each_flow(lambda offset: base(offset, 0).wait())
        return

    def greet_flow(index, total):
        away = reach - index // 2
        offset = jnp.where(lax.rem(index, 2) == 0, reach + away, reach - away)
        begun = origin(offset)
        here, there = hot(me, offset), hot(begun, offset)

        def greet_part(part, total):
            source = beside(part) * inner + y
            middleman = hot(source, offset)

            @pl.when(here | middleman)
            def _():
                greet((beside(part), y))

            @pl.when(middleman)
            def _():
                greet(place(shifted(source, offset)))

            @pl.when(there)
            def _():
                greet((flip(begun // inner, part, outer), lax.rem(begun, inner)))

            return (total + jnp.where(here | middleman, 1, 0) + jnp.where(middleman, 1, 0)
                    + jnp.where(there, 1, 0))

        return lax.fori_loop(1, parts, greet_part, total)

    pl.semaphore_wait(barrier, lax.fori_loop(0, 2 * reach, greet_flow, 2 * reach))

    def start_hot(offset):
        @pl.when(hot(me, offset))
        def _():
            each_part(lambda part: detour(offset, part).start())
            direct(offset).start()

        @pl.when(close(me, offset))
        def _():
            whole(offset).start()

    def middle(offset, act):
        def one(part):
            source = beside(part) * inner + y

            @pl.when(hot(source, offset))
            def _():
                act(offset, part, source)

        each_part(one)

    def pass_on(offset, part, source):
        detour(offset, part).wait_recv()
        forward(offset, part, source).start()

    def finish(offset):
        repeat(0, 2, lambda step: base(offset, step).wait())

        @pl.when(close(me, offset))
        def _():
            whole(offset).wait_send()

        @pl.when(close(origin(offset), offset))
        def _():
            whole(offset).wait_recv()

        @pl.when(hot(me, offset))
        def _():
            direct(offset).wait_send()
            each_part(lambda part: detour(offset, part).wait_send())

        @pl.when(hot(origin(offset), offset))
        def _():
            direct(offset).wait_recv()
            each_part(lambda part: forward(offset, part, me).wait_recv())

        middle(offset, lambda offset, part, source: forward(offset, part, source).wait_send())

    def batch_step(step):
        each_flow(lambda offset: base(offset, step).start())

        @pl.when(step == 0)
        def _():
            each_flow(lambda offset: middle(offset, pass_on))

    each_flow(start_hot)
    repeat(0, 2, batch_step)
    each_flow(finish)


def settle_kernel(meta_ref, own_ref, low_ref, high_ref, out_ref, meta, total, out_buf,
                  load_sem, out_sem):
    num_off, first = low_ref.shape[0], low_ref.shape[1]
    reach = num_off // 2
    num_kinds, num_steps = out_ref.shape[0], out_ref.shape[1]
    blocks, _, block_rows = total.shape
    load = pltpu.make_async_copy(meta_ref, meta, load_sem)
    load.start()

    def clear(block, carry):
        total[block] = jnp.zeros_like(total[block])
        return carry

    lax.fori_loop(0, blocks, clear, 0, unroll=4)
    load.wait()

    def add(offset, slot, value):
        row = meta[offset, 0, 0, slot]
        total[row] = total[row] + value

    def one_flow(offset, carry):
        live = meta[offset, 1, 0, 0]

        def low_slot(slot, carry):
            add(offset, slot, low_ref[offset, slot])
            return carry

        def high_slot(slot, carry):
            add(offset, slot, high_ref[offset, slot - first])
            return carry

        @pl.when(offset != reach)
        def _():
            lax.fori_loop(0, jnp.minimum(live, first), low_slot, 0)
            lax.fori_loop(first, live, high_slot, 0)

        return carry

    def own_slot(slot, carry):
        add(reach, slot, own_ref[slot])
        return carry

    lax.fori_loop(0, num_off, one_flow, 0)
    lax.fori_loop(0, meta[reach, 1, 0, 0], own_slot, 0)

    per_cut = blocks // OUT_CUTS
    stores = []
    for cut in range(OUT_CUTS):
        def one_block(block, carry):
            lanes = pl.ds(pl.multiple_of(block * block_rows, block_rows), block_rows)
            out_buf[:, :, lanes] = total[block].reshape(num_kinds, num_steps, block_rows)
            return carry

        lax.fori_loop(cut * per_cut, (cut + 1) * per_cut, one_block, 0, unroll=2)
        lanes = pl.ds(cut * per_cut * block_rows, per_cut * block_rows)
        store = pltpu.make_async_copy(
            out_buf.at[:, :, lanes], out_ref.at[:, :, lanes], out_sem.at[cut])
        store.start()
        stores.append(store)
    for store in stores:
        store.wait()


def on_device(axes, sizes, atm_blocks, tile_flux, tile_frac, weights, block_row, block_col,
              send_counts):
    num_steps, num_kinds = tile_flux.shape[0], tile_flux.shape[1]
    num_flux = num_steps * num_kinds
    num_off, slots, block_rows, block_cols = weights.shape[1:]
    tiles = tile_flux.shape[2]
    land_blocks = tile_flux.shape[3] // block_cols
    rows = block_row.transpose(1, 0, 2)
    columns = block_col.transpose(1, 0, 2)
    count = sizes[0] * sizes[1]
    half, first = slots // 2, slots // 4
    parts = 4 if sizes[0] % 4 == 0 else 1
    piece = (slots - half) // parts
    classes = min(count, MAX_CLASSES)

    vmem = pl.BlockSpec(memory_space=pltpu.VMEM)
    smem = pl.BlockSpec(memory_space=pltpu.SMEM)
    hbm = pl.BlockSpec(memory_space=pltpu.HBM)
    dma = pltpu.SemaphoreType.DMA
    steps = 2 * slots * num_off
    part, own, low, arrived_meta, pick = pl.pallas_call(
        functools.partial(exchange_kernel, axes, sizes, classes, first, half),
        out_shape=(
            pltpu.VMEM((num_off, slots, num_flux, block_rows), jnp.float32),
            pltpu.VMEM((slots, num_flux, block_rows), jnp.float32),
            pltpu.VMEM((num_off, first, num_flux, block_rows), jnp.float32),
            pltpu.VMEM((num_off, 2, 1, slots), jnp.int32),
            jax.ShapeDtypeStruct((1,), jnp.int32),
        ),
        in_specs=[hbm, hbm, smem, smem, hbm, hbm],
        out_specs=(vmem, vmem, vmem, vmem, smem),
        scratch_shapes=[
            pltpu.VMEM((land_blocks, num_steps, num_kinds, tiles, block_cols), tile_flux.dtype),
            pltpu.VMEM((land_blocks, tiles, block_cols), tile_frac.dtype),
            pltpu.VMEM(weights.shape[1:], weights.dtype),
            pltpu.VMEM((num_off, 2, 1, slots), jnp.int32),
            pltpu.VMEM((sizes[0], 1, LANES), jnp.int32),
            pltpu.VMEM((sizes[1], 1, LANES), jnp.int32),
            dma((land_blocks,)),
            dma((land_blocks,)),
            dma((steps,)),
            dma((num_off,)),
            dma,
            dma((num_off, first)),
            dma((num_off, first)),
            dma((num_off,)),
            dma((num_off,)),
            dma((sizes[0],)),
            dma((sizes[0],)),
            dma((sizes[1],)),
            dma((sizes[1],)),
        ],
        compiler_params=pltpu.CompilerParams(collective_id=0, has_side_effects=True,
                                             vmem_limit_bytes=55 * 2**20),
        name="exchange",
    )(tile_flux, tile_frac, columns, send_counts, rows, weights[0])

    def settle(arrived_meta, own, low, high):
        return pl.pallas_call(
            settle_kernel,
            out_shape=jax.ShapeDtypeStruct((num_kinds, num_steps, atm_blocks * block_rows),
                                           jnp.float32),
            in_specs=[vmem] * 4,
            out_specs=hbm,
            scratch_shapes=[
                pltpu.SMEM((num_off, 2, 1, slots), jnp.int32),
                pltpu.VMEM((atm_blocks, num_flux, block_rows), jnp.float32),
                pltpu.VMEM((num_kinds, num_steps, atm_blocks * block_rows), jnp.float32),
                dma,
                dma((OUT_CUTS,)),
            ],
            compiler_params=pltpu.CompilerParams(vmem_limit_bytes=16 * 2**20),
            name="settle",
        )(arrived_meta, own, low, high)

    def rest(group):
        def call(part, arrived_meta, own, low):
            high = pl.pallas_call(
                functools.partial(rest_kernel, axes, sizes, classes, group, first, half, parts),
                out_shape=pltpu.VMEM((num_off, slots - first, num_flux, block_rows),
                                     jnp.float32),
                in_specs=[vmem],
                out_specs=vmem,
                scratch_shapes=[
                    pltpu.VMEM((num_off, parts, piece, num_flux, block_rows), jnp.float32),
                ] + [dma((num_off, 2))] * 2 + [dma((num_off,))] * 2 + [dma((num_off, parts))] * 4,
                compiler_params=pltpu.CompilerParams(
                    collective_id=classes + 1 if group is None else 1 + group,
                    has_side_effects=True, vmem_limit_bytes=16 * 2**20),
                name="rest",
            )(part)
            return settle(arrived_meta, own, low, high)
        return call

    groups = list(range(classes)) + [None]
    out = lax.switch(pick[0], [rest(group) for group in groups],
                     part, arrived_meta, own, low)
    return out.transpose(1, 0, 2)


def solution(mesh):
    axes = ("gx", "gy")
    sizes = (mesh.shape["gx"], mesh.shape["gy"])
    return jax.shard_map(
        functools.partial(on_device, axes, sizes, AB_DEV),
        mesh=mesh,
        in_specs=(
            P(None, None, None, ("gx", "gy")),
            P(None, ("gx", "gy")),
            P(("gx", "gy"), None, None, None, None),
            P(("gx", "gy"), None, None),
            P(("gx", "gy"), None, None),
            P(("gx", "gy"), None),
        ),
        out_specs=P(None, None, ("gx", "gy")),
        check_vma=False,
    )
```

```python
import functools

import jax
import jax.numpy as jnp
from jax import lax
from jax.experimental import pallas as pl
from jax.experimental.pallas import tpu as pltpu
from jax.sharding import PartitionSpec as P

OUT_CUTS = 4
EARLY = 4
MAX_CLASSES = 32
CORES = 2
LANES = 128
AB_DEV = 48


def ranges(begin, end, sizes):
    spans = []
    for size in sizes:
        size = min(size, end - begin)
        if size > 0:
            spans.append((begin, size))
            begin += size
    if begin < end:
        spans.append((begin, end - begin))
    return spans


def flow_order(reach):
    order = []
    for away in range(reach, 0, -1):
        order += [reach + away, reach - away]
    return order


def flip(index, bits, size):
    out, weight = index, 1
    while weight < size:
        mine, theirs = lax.rem(index // weight, 2), lax.rem(bits // weight, 2)
        out = out + weight * theirs * (1 - 2 * mine)
        weight *= 2
    return out


def exchange_kernel(axes, sizes, classes, first, half, flux_ref, frac_ref, col_ref, count_ref, rows_ref,
                    weights_ref, part_ref, own_ref, arrived_ref, arrived_meta_ref, pick_ref,
                    flux_buf, frac_buf, weights_buf, meta, column_votes, row_votes,
                    flux_sem, frac_sem, weight_sem, meta_sem, own_sem, send_sem, recv_sem,
                    meta_send_sem, meta_recv_sem, column_send_sem, column_recv_sem,
                    row_send_sem, row_recv_sem):
    num_off, slots = weights_buf.shape[0], weights_buf.shape[1]
    num_steps, num_kinds, tiles, _ = flux_ref.shape
    cols = weights_buf.shape[3]
    reach = num_off // 2
    outer, inner = sizes
    count = outer * inner
    x, y = lax.axis_index(axes[0]), lax.axis_index(axes[1])
    me = x * inner + y
    first_spans = ranges(0, first, (1, 1, 2))
    later_spans = ranges(first, slots, (half - first,))

    def place(there):
        return (there // inner, lax.rem(there, inner))

    def target(offset):
        return lax.rem(me + offset - reach + count, count)

    def steps(size, act):
        def one(step, carry):
            act(step)
            return carry

        lax.fori_loop(1, size, one, 0)

    barrier = pltpu.get_barrier_semaphore()
    greeted = 2 * reach + outer - 1 + inner - 1

    def greet(device):
        pl.semaphore_signal(barrier, inc=1, device_id=device,
                            device_id_type=pl.DeviceIdType.MESH)

    for offset in flow_order(reach):
        greet(place(target(offset)))
    steps(outer, lambda step: greet((lax.rem(x + step, outer), y)))
    steps(inner, lambda step: greet((x, lax.rem(y + step, inner))))

    def repeat(begin, end, act):
        def one(step, carry):
            act(step)
            return carry

        lax.fori_loop(begin, end, one, 0)

    def flow_offset(index):
        away = reach - index // 2
        return jnp.where(lax.rem(index, 2) == 0, reach + away, reach - away)

    def land_loads(block):
        lanes = pl.ds(pl.multiple_of(block * cols, cols), cols)
        return (pltpu.make_async_copy(flux_ref.at[:, :, :, lanes], flux_buf.at[block],
                                      flux_sem.at[block]),
                pltpu.make_async_copy(frac_ref.at[:, lanes], frac_buf.at[block],
                                      frac_sem.at[block]))

    def start_land(block):
        for load in land_loads(block):
            load.start()

    def wait_land(block):
        for load in land_loads(block):
            load.wait()

    def meta_load(offset):
        return pltpu.make_async_copy(rows_ref.at[offset], meta.at[offset, 0],
                                     meta_sem.at[offset])

    spans = first_spans + later_spans

    def weight_load(offset, chunk):
        span = pl.ds(*spans[chunk])
        return pltpu.make_async_copy(weights_ref.at[offset, span], weights_buf.at[offset, span],
                                     weight_sem.at[offset, chunk])

    def own_load():
        return pltpu.make_async_copy(weights_ref.at[reach], weights_buf.at[reach],
                                     weight_sem.at[reach, 0])

    repeat(0, flux_buf.shape[0], start_land)
    repeat(0, num_off, lambda offset: meta_load(offset).start())
    repeat(0, EARLY, lambda index: weight_load(flow_offset(index), 0).start())

    lane = lax.broadcasted_iota(jnp.int32, (1, LANES), 1)
    mine = lax.rem(me, classes)
    vote = jnp.where(lane <= classes, 1, 0)
    for offset in range(num_off):
        live = count_ref[0, offset]
        meta[offset, 1] = jnp.full((1, slots), live, jnp.int32)
        if offset != reach:
            theirs = lax.rem(target(offset), classes)
            fits = (lane == mine) | (lane == theirs) | (lane >= classes) | (live <= half)
            vote = jnp.where(fits, vote, 0)
    column_votes[x] = vote

    repeat(0, flux_buf.shape[0], wait_land)
    repeat(EARLY, 2 * reach, lambda index: weight_load(flow_offset(index), 0).start())
    for chunk in range(1, len(spans)):
        repeat(0, 2 * reach, lambda index, chunk=chunk: weight_load(
            flow_offset(index), chunk).start())
    own_load().start()

    def column_vote(step, source):
        return pltpu.make_async_remote_copy(
            src_ref=column_votes.at[x], dst_ref=column_votes.at[source],
            send_sem=column_send_sem.at[step], recv_sem=column_recv_sem.at[step],
            device_id=(lax.rem(x + step, outer), y), device_id_type=pl.DeviceIdType.MESH)

    def row_vote(step, source):
        return pltpu.make_async_remote_copy(
            src_ref=row_votes.at[y], dst_ref=row_votes.at[source],
            send_sem=row_send_sem.at[step], recv_sem=row_recv_sem.at[step],
            device_id=(x, lax.rem(y + step, inner)), device_id_type=pl.DeviceIdType.MESH)

    def product(offset, slot):
        block = col_ref[offset, 0, slot]
        frac = frac_buf[block]
        flux = flux_buf[block].astype(jnp.float32)
        flux = jnp.stack([flux[step] for step in range(num_steps)], axis=1)
        flux = flux.reshape(num_steps * num_kinds, tiles, cols)
        merged = jnp.sum(flux * frac[None], axis=1) / jnp.sum(frac, axis=0, keepdims=True)
        return lax.dot_general(merged.astype(jnp.bfloat16), weights_buf[offset, slot],
                               (((1,), (1,)), ((), ())), preferred_element_type=jnp.float32)

    def chunk_copy(offset, chunk):
        span = pl.ds(*spans[chunk])
        return pltpu.make_async_remote_copy(
            src_ref=part_ref.at[offset, span], dst_ref=arrived_ref.at[offset, span],
            send_sem=send_sem.at[offset, chunk], recv_sem=recv_sem.at[offset, chunk],
            device_id=place(target(offset)), device_id_type=pl.DeviceIdType.MESH)

    def meta_copy(offset):
        return pltpu.make_async_remote_copy(
            src_ref=meta.at[offset], dst_ref=arrived_meta_ref.at[offset],
            send_sem=meta_send_sem.at[offset], recv_sem=meta_recv_sem.at[offset],
            device_id=place(target(offset)), device_id_type=pl.DeviceIdType.MESH)

    own_meta = pltpu.make_async_copy(meta.at[reach], arrived_meta_ref.at[reach], own_sem)

    def store_slots(offset, chunk):
        begin, size = spans[chunk]

        def one_slot(slot, carry):
            part_ref[offset, slot] = product(offset, slot)
            return carry

        weight_load(offset, chunk).wait()
        lax.fori_loop(begin, begin + size, one_slot, 0, unroll=2 if size % 2 == 0 else 1)

    def send_chunk(chunk, index):
        offset = flow_offset(index)
        store_slots(offset, chunk)
        chunk_copy(offset, chunk).start()
        if chunk == 0:
            meta_copy(offset).start()

    store_slots(2 * reach, 0)
    repeat(0, num_off, lambda offset: meta_load(offset).wait())
    pl.semaphore_wait(barrier, greeted)
    chunk_copy(2 * reach, 0).start()
    meta_copy(2 * reach).start()
    own_meta.start()
    steps(outer, lambda step: column_vote(step, x).start())
    for chunk in range(len(first_spans)):
        repeat(1 if chunk == 0 else 0, 2 * reach,
               lambda index, chunk=chunk: send_chunk(chunk, index))
        if chunk == min(1, len(first_spans) - 1):
            steps(outer, lambda step: column_vote(
                step, lax.rem(x - step + outer, outer)).wait())
            row_votes[y] = jnp.min(column_votes[:, 0, :], axis=0, keepdims=True)
            steps(inner, lambda step: row_vote(step, y).start())
    for chunk in range(len(first_spans), len(spans)):
        repeat(0, 2 * reach, lambda index, chunk=chunk: store_slots(flow_offset(index), chunk))

    def own_slot(slot, carry):
        own_ref[slot] = product(reach, slot)
        return carry

    own_load().wait()
    lax.fori_loop(0, slots, own_slot, 0, unroll=2)
    steps(inner, lambda step: row_vote(step, lax.rem(y - step + inner, inner)).wait())
    agreed = jnp.min(row_votes[:, 0, :], axis=0, keepdims=True)
    pick_ref[0] = jnp.min(jnp.where((agreed > 0) & (lane <= classes), lane, classes))
    own_meta.wait()
    for chunk in range(len(first_spans)):
        repeat(0, 2 * reach, lambda index, chunk=chunk: chunk_copy(
            flow_offset(index), chunk).wait())
    repeat(0, 2 * reach, lambda index: meta_copy(flow_offset(index)).wait())


def rest_kernel(axes, sizes, classes, group, first, half, parts, part_ref, arrived_ref, relay,
                base_send, base_recv, send_sem, recv_sem, pass_send, pass_recv,
                fwd_send, fwd_recv):
    num_off, slots = part_ref.shape[0], part_ref.shape[1]
    reach = num_off // 2
    outer, inner = sizes
    count = outer * inner
    x, y = lax.axis_index(axes[0]), lax.axis_index(axes[1])
    me = x * inner + y
    batch = (half - first) // 2
    piece = (slots - half) // parts

    def place(there):
        return (there // inner, lax.rem(there, inner))

    def shifted(device, offset):
        return lax.rem(device + offset - reach + count, count)

    def origin(offset):
        return lax.rem(me - offset + reach + count, count)

    def beside(part):
        return flip(x, part, outer)

    def remote(src, dst, send, recv, device):
        return pltpu.make_async_remote_copy(
            src_ref=src, dst_ref=dst, send_sem=send, recv_sem=recv,
            device_id=device, device_id_type=pl.DeviceIdType.MESH)

    def member(device):
        return (device if classes == count else lax.rem(device, classes)) == group

    def heavy(source, goal):
        return member(source) | member(goal)

    def near(source, goal):
        return source // CORES == goal // CORES

    def hot(source, offset):
        goal = shifted(source, offset)
        return heavy(source, goal) & jnp.logical_not(near(source, goal))

    def close(source, offset):
        goal = shifted(source, offset)
        return heavy(source, goal) & near(source, goal)

    def repeat(begin, end, act):
        def one(step, carry):
            act(step)
            return carry

        lax.fori_loop(begin, end, one, 0)

    def each_flow(act):
        def one(index):
            away = reach - index // 2
            act(jnp.where(lax.rem(index, 2) == 0, reach + away, reach - away))

        repeat(0, 2 * reach, one)

    def each_part(act):
        repeat(1, parts, act)

    anyone = (lax.rem(x + 1, outer), y)

    def toward(offset):
        return place(shifted(me, offset))

    def span(offset, begin, size, send, recv, device):
        return remote(part_ref.at[offset, pl.ds(begin, size)],
                      arrived_ref.at[offset, pl.ds(begin - first, size)],
                      send, recv, device)

    def base(offset, step, device=anyone):
        size = slots - first if group is None else batch
        return span(offset, first + step * batch, size, base_send.at[offset, step],
                    base_recv.at[offset, step], device)

    def direct(offset, device=anyone):
        return span(offset, half, piece, send_sem.at[offset], recv_sem.at[offset], device)

    def whole(offset, device=anyone):
        return span(offset, half, slots - half, send_sem.at[offset], recv_sem.at[offset],
                    device)

    def detour(offset, part, device=anyone):
        return remote(part_ref.at[offset, pl.ds(half + part * piece, piece)],
                      relay.at[offset, part], pass_send.at[offset, part],
                      pass_recv.at[offset, part], device)

    def forward(offset, part, device=anyone):
        return remote(relay.at[offset, part],
                      arrived_ref.at[offset, pl.ds(half - first + part * piece, piece)],
                      fwd_send.at[offset, part], fwd_recv.at[offset, part], device)

    barrier = pltpu.get_barrier_semaphore()

    def greet(device, inc=1):
        pl.semaphore_signal(barrier, inc=inc, device_id=device,
                            device_id_type=pl.DeviceIdType.MESH)

    each_flow(lambda offset: greet(place(shifted(me, offset))))
    if group is None:
        pl.semaphore_wait(barrier, 2 * reach)
        each_flow(lambda offset: base(offset, 0, toward(offset)).start())
        each_flow(lambda offset: base(offset, 0).wait())
        return

    def greet_flow(index, total):
        away = reach - index // 2
        offset = jnp.where(lax.rem(index, 2) == 0, reach + away, reach - away)
        begun = origin(offset)
        here, there = hot(me, offset), hot(begun, offset)

        def greet_part(part, total):
            source = beside(part) * inner + y
            middleman = hot(source, offset)

            @pl.when(here | middleman)
            def _():
                greet((beside(part), y))

            @pl.when(middleman)
            def _():
                greet(place(shifted(source, offset)))

            @pl.when(there)
            def _():
                greet((flip(begun // inner, part, outer), lax.rem(begun, inner)))

            return (total + jnp.where(here | middleman, 1, 0) + jnp.where(middleman, 1, 0)
                    + jnp.where(there, 1, 0))

        return lax.fori_loop(1, parts, greet_part, total)

    pl.semaphore_wait(barrier, lax.fori_loop(0, 2 * reach, greet_flow, 2 * reach))

    def start_hot(offset):
        @pl.when(hot(me, offset))
        def _():
            each_part(lambda part: detour(offset, part, (beside(part), y)).start())
            direct(offset, toward(offset)).start()

        @pl.when(close(me, offset))
        def _():
            whole(offset, toward(offset)).start()

    def middle(offset, act):
        def one(part):
            source = beside(part) * inner + y

            @pl.when(hot(source, offset))
            def _():
                act(offset, part, source)

        each_part(one)

    def pass_on(offset, part, source):
        detour(offset, part).wait_recv()
        forward(offset, part, place(shifted(source, offset))).start()

    def finish(offset):
        repeat(0, 2, lambda step: base(offset, step).wait())

        @pl.when(close(me, offset))
        def _():
            whole(offset).wait_send()

        @pl.when(close(origin(offset), offset))
        def _():
            whole(offset).wait_recv()

        @pl.when(hot(me, offset))
        def _():
            direct(offset).wait_send()
            each_part(lambda part: detour(offset, part).wait_send())

        @pl.when(hot(origin(offset), offset))
        def _():
            direct(offset).wait_recv()
            each_part(lambda part: forward(offset, part).wait_recv())

        middle(offset, lambda offset, part, source: forward(offset, part).wait_send())

    def batch_step(step):
        each_flow(lambda offset: base(offset, step, toward(offset)).start())

        @pl.when(step == 0)
        def _():
            each_flow(lambda offset: middle(offset, pass_on))

    each_flow(start_hot)
    repeat(0, 2, batch_step)
    each_flow(finish)


def settle_kernel(meta_ref, own_ref, low_ref, high_ref, out_ref, meta, total, out_buf,
                  load_sem, out_sem):
    num_off, first = low_ref.shape[0], low_ref.shape[1]
    reach = num_off // 2
    num_kinds, num_steps = out_ref.shape[0], out_ref.shape[1]
    blocks, _, block_rows = total.shape
    load = pltpu.make_async_copy(meta_ref, meta, load_sem)
    load.start()

    def clear(block, carry):
        total[block] = jnp.zeros_like(total[block])
        return carry

    lax.fori_loop(0, blocks, clear, 0, unroll=4)
    load.wait()

    def add_pair(offset, slot, end, source, shift):
        lone = slot + 1 >= end
        other = jnp.where(lone, slot, slot + 1)
        row, next_row = meta[offset, 0, 0, slot], meta[offset, 0, 0, other]
        value, next_value = source(slot - shift), source(other - shift)
        old, next_old = total[row], total[next_row]
        new = old + value
        kept = jnp.where(row == next_row, new, next_old)
        total[row] = new
        total[next_row] = jnp.where(lone, kept, kept + next_value)

    def add_all(offset, begin, end, source, shift):
        def one(pair, carry):
            add_pair(offset, begin + 2 * pair, end, source, shift)
            return carry

        lax.fori_loop(0, (end - begin + 1) // 2, one, 0)

    def one_flow(offset, carry):
        live = meta[offset, 1, 0, 0]

        @pl.when(offset != reach)
        def _():
            add_all(offset, 0, jnp.minimum(live, first), lambda slot: low_ref[offset, slot], 0)
            add_all(offset, first, jnp.maximum(live, first),
                    lambda slot: high_ref[offset, slot], first)

        return carry

    lax.fori_loop(0, num_off, one_flow, 0)
    add_all(reach, 0, meta[reach, 1, 0, 0], lambda slot: own_ref[slot], 0)

    per_cut = blocks // OUT_CUTS
    stores = []
    for cut in range(OUT_CUTS):
        def one_block(block, carry):
            lanes = pl.ds(pl.multiple_of(block * block_rows, block_rows), block_rows)
            out_buf[:, :, lanes] = total[block].reshape(num_kinds, num_steps, block_rows)
            return carry

        lax.fori_loop(cut * per_cut, (cut + 1) * per_cut, one_block, 0, unroll=2)
        lanes = pl.ds(cut * per_cut * block_rows, per_cut * block_rows)
        store = pltpu.make_async_copy(
            out_buf.at[:, :, lanes], out_ref.at[:, :, lanes], out_sem.at[cut])
        store.start()
        stores.append(store)
    for store in stores:
        store.wait()


def on_device(axes, sizes, atm_blocks, tile_flux, tile_frac, weights, block_row, block_col,
              send_counts):
    num_steps, num_kinds = tile_flux.shape[0], tile_flux.shape[1]
    num_flux = num_steps * num_kinds
    num_off, slots, block_rows, block_cols = weights.shape[1:]
    tiles = tile_flux.shape[2]
    land_blocks = tile_flux.shape[3] // block_cols
    rows = block_row.transpose(1, 0, 2)
    columns = block_col.transpose(1, 0, 2)
    count = sizes[0] * sizes[1]
    half, first = slots // 2, slots // 4
    parts = 4 if sizes[0] % 4 == 0 else 1
    piece = (slots - half) // parts
    classes = min(count, MAX_CLASSES)

    vmem = pl.BlockSpec(memory_space=pltpu.VMEM)
    smem = pl.BlockSpec(memory_space=pltpu.SMEM)
    hbm = pl.BlockSpec(memory_space=pltpu.HBM)
    dma = pltpu.SemaphoreType.DMA
    part, own, low, arrived_meta, pick = pl.pallas_call(
        functools.partial(exchange_kernel, axes, sizes, classes, first, half),
        out_shape=(
            pltpu.VMEM((num_off, slots, num_flux, block_rows), jnp.float32),
            pltpu.VMEM((slots, num_flux, block_rows), jnp.float32),
            pltpu.VMEM((num_off, first, num_flux, block_rows), jnp.float32),
            pltpu.VMEM((num_off, 2, 1, slots), jnp.int32),
            jax.ShapeDtypeStruct((1,), jnp.int32),
        ),
        in_specs=[hbm, hbm, smem, smem, hbm, hbm],
        out_specs=(vmem, vmem, vmem, vmem, smem),
        scratch_shapes=[
            pltpu.VMEM((land_blocks, num_steps, num_kinds, tiles, block_cols), tile_flux.dtype),
            pltpu.VMEM((land_blocks, tiles, block_cols), tile_frac.dtype),
            pltpu.VMEM(weights.shape[1:], weights.dtype),
            pltpu.VMEM((num_off, 2, 1, slots), jnp.int32),
            pltpu.VMEM((sizes[0], 1, LANES), jnp.int32),
            pltpu.VMEM((sizes[1], 1, LANES), jnp.int32),
            dma((land_blocks,)),
            dma((land_blocks,)),
            dma((num_off, slots)),
            dma((num_off,)),
            dma,
            dma((num_off, first)),
            dma((num_off, first)),
            dma((num_off,)),
            dma((num_off,)),
            dma((sizes[0],)),
            dma((sizes[0],)),
            dma((sizes[1],)),
            dma((sizes[1],)),
        ],
        compiler_params=pltpu.CompilerParams(collective_id=0, has_side_effects=True,
                                             vmem_limit_bytes=55 * 2**20),
        name="exchange",
    )(tile_flux, tile_frac, columns, send_counts, rows, weights[0])

    def settle(arrived_meta, own, low, high):
        return pl.pallas_call(
            settle_kernel,
            out_shape=jax.ShapeDtypeStruct((num_kinds, num_steps, atm_blocks * block_rows),
                                           jnp.float32),
            in_specs=[vmem] * 4,
            out_specs=hbm,
            scratch_shapes=[
                pltpu.SMEM((num_off, 2, 1, slots), jnp.int32),
                pltpu.VMEM((atm_blocks, num_flux, block_rows), jnp.float32),
                pltpu.VMEM((num_kinds, num_steps, atm_blocks * block_rows), jnp.float32),
                dma,
                dma((OUT_CUTS,)),
            ],
            compiler_params=pltpu.CompilerParams(vmem_limit_bytes=16 * 2**20),
            name="settle",
        )(arrived_meta, own, low, high)

    def rest(group):
        def call(part, arrived_meta, own, low):
            high = pl.pallas_call(
                functools.partial(rest_kernel, axes, sizes, classes, group, first, half, parts),
                out_shape=pltpu.VMEM((num_off, slots - first, num_flux, block_rows),
                                     jnp.float32),
                in_specs=[vmem],
                out_specs=vmem,
                scratch_shapes=[
                    pltpu.VMEM((num_off, parts, piece, num_flux, block_rows), jnp.float32),
                ] + [dma((num_off, 2))] * 2 + [dma((num_off,))] * 2 + [dma((num_off, parts))] * 4,
                compiler_params=pltpu.CompilerParams(
                    collective_id=classes + 1 if group is None else 1 + group,
                    has_side_effects=True, vmem_limit_bytes=16 * 2**20),
                name="rest",
            )(part)
            return settle(arrived_meta, own, low, high)
        return call

    groups = list(range(classes)) + [None]
    out = lax.switch(pick[0], [rest(group) for group in groups],
                     part, arrived_meta, own, low)
    return out.transpose(1, 0, 2)


def solution(mesh):
    axes = ("gx", "gy")
    sizes = (mesh.shape["gx"], mesh.shape["gy"])
    return jax.shard_map(
        functools.partial(on_device, axes, sizes, AB_DEV),
        mesh=mesh,
        in_specs=(
            P(None, None, None, ("gx", "gy")),
            P(None, ("gx", "gy")),
            P(("gx", "gy"), None, None, None, None),
            P(("gx", "gy"), None, None),
            P(("gx", "gy"), None, None),
            P(("gx", "gy"), None),
        ),
        out_specs=P(None, None, ("gx", "gy")),
        check_vma=False,
    )
```

```python
import functools

import jax
import jax.numpy as jnp
from jax import lax
from jax.experimental import pallas as pl
from jax.experimental.pallas import tpu as pltpu
from jax.sharding import PartitionSpec as P

OUT_CUTS = 6
EARLY = 4
MAX_CLASSES = 32
CORES = 2
LANES = 128
AB_DEV = 48


def ranges(begin, end, sizes):
    spans = []
    for size in sizes:
        size = min(size, end - begin)
        if size > 0:
            spans.append((begin, size))
            begin += size
    if begin < end:
        spans.append((begin, end - begin))
    return spans


def flow_order(reach):
    order = []
    for away in range(reach, 0, -1):
        order += [reach + away, reach - away]
    return order


def flip(index, bits, size):
    out, weight = index, 1
    while weight < size:
        mine, theirs = lax.rem(index // weight, 2), lax.rem(bits // weight, 2)
        out = out + weight * theirs * (1 - 2 * mine)
        weight *= 2
    return out


def exchange_kernel(axes, sizes, classes, first, half, flux_ref, frac_ref, col_ref, count_ref, rows_ref,
                    weights_ref, part_ref, own_ref, arrived_ref, arrived_meta_ref, pick_ref,
                    flux_buf, frac_buf, weights_buf, meta, column_votes, row_votes,
                    flux_sem, frac_sem, weight_sem, meta_sem, own_sem, send_sem, recv_sem,
                    meta_send_sem, meta_recv_sem, column_send_sem, column_recv_sem,
                    row_send_sem, row_recv_sem):
    num_off, slots = weights_buf.shape[0], weights_buf.shape[1]
    num_steps, num_kinds, tiles, _ = flux_ref.shape
    cols = weights_buf.shape[3]
    reach = num_off // 2
    outer, inner = sizes
    count = outer * inner
    x, y = lax.axis_index(axes[0]), lax.axis_index(axes[1])
    me = x * inner + y
    first_spans = ranges(0, first, (1, 1, 2))
    later_spans = ranges(first, slots, (half - first,))

    def place(there):
        return (there // inner, lax.rem(there, inner))

    def target(offset):
        return lax.rem(me + offset - reach + count, count)

    def steps(size, act):
        def one(step, carry):
            act(step)
            return carry

        lax.fori_loop(1, size, one, 0)

    barrier = pltpu.get_barrier_semaphore()
    greeted = 2 * reach + outer - 1 + inner - 1

    def greet(device):
        pl.semaphore_signal(barrier, inc=1, device_id=device,
                            device_id_type=pl.DeviceIdType.MESH)

    for offset in flow_order(reach):
        greet(place(target(offset)))
    steps(outer, lambda step: greet((lax.rem(x + step, outer), y)))
    steps(inner, lambda step: greet((x, lax.rem(y + step, inner))))

    def repeat(begin, end, act):
        def one(step, carry):
            act(step)
            return carry

        lax.fori_loop(begin, end, one, 0)

    def flow_offset(index):
        away = reach - index // 2
        return jnp.where(lax.rem(index, 2) == 0, reach + away, reach - away)

    def land_loads(block):
        lanes = pl.ds(pl.multiple_of(block * cols, cols), cols)
        return (pltpu.make_async_copy(flux_ref.at[:, :, :, lanes], flux_buf.at[block],
                                      flux_sem.at[block]),
                pltpu.make_async_copy(frac_ref.at[:, lanes], frac_buf.at[block],
                                      frac_sem.at[block]))

    def start_land(block):
        for load in land_loads(block):
            load.start()

    def wait_land(block):
        for load in land_loads(block):
            load.wait()

    def meta_load(offset):
        return pltpu.make_async_copy(rows_ref.at[offset], meta.at[offset, 0],
                                     meta_sem.at[offset])

    spans = first_spans + later_spans

    def weight_load(offset, chunk):
        span = pl.ds(*spans[chunk])
        return pltpu.make_async_copy(weights_ref.at[offset, span], weights_buf.at[offset, span],
                                     weight_sem.at[offset, chunk])

    def own_load():
        return pltpu.make_async_copy(weights_ref.at[reach], weights_buf.at[reach],
                                     weight_sem.at[reach, 0])

    repeat(0, flux_buf.shape[0], start_land)
    repeat(0, num_off, lambda offset: meta_load(offset).start())
    repeat(0, EARLY, lambda index: weight_load(flow_offset(index), 0).start())

    lane = lax.broadcasted_iota(jnp.int32, (1, LANES), 1)
    mine = lax.rem(me, classes)
    vote = jnp.where(lane <= classes, 1, 0)
    for offset in range(num_off):
        live = count_ref[0, offset]
        meta[offset, 1] = jnp.full((1, slots), live, jnp.int32)
        if offset != reach:
            theirs = lax.rem(target(offset), classes)
            fits = (lane == mine) | (lane == theirs) | (lane >= classes) | (live <= half)
            vote = jnp.where(fits, vote, 0)
    column_votes[x] = vote

    repeat(0, flux_buf.shape[0], wait_land)
    repeat(EARLY, 2 * reach, lambda index: weight_load(flow_offset(index), 0).start())
    for chunk in range(1, len(spans)):
        repeat(0, 2 * reach, lambda index, chunk=chunk: weight_load(
            flow_offset(index), chunk).start())
    own_load().start()

    def column_vote(step, source):
        return pltpu.make_async_remote_copy(
            src_ref=column_votes.at[x], dst_ref=column_votes.at[source],
            send_sem=column_send_sem.at[step], recv_sem=column_recv_sem.at[step],
            device_id=(lax.rem(x + step, outer), y), device_id_type=pl.DeviceIdType.MESH)

    def row_vote(step, source):
        return pltpu.make_async_remote_copy(
            src_ref=row_votes.at[y], dst_ref=row_votes.at[source],
            send_sem=row_send_sem.at[step], recv_sem=row_recv_sem.at[step],
            device_id=(x, lax.rem(y + step, inner)), device_id_type=pl.DeviceIdType.MESH)

    def product(offset, slot):
        block = col_ref[offset, 0, slot]
        frac = frac_buf[block]
        flux = flux_buf[block].astype(jnp.float32)
        flux = jnp.stack([flux[step] for step in range(num_steps)], axis=1)
        flux = flux.reshape(num_steps * num_kinds, tiles, cols)
        merged = jnp.sum(flux * frac[None], axis=1) / jnp.sum(frac, axis=0, keepdims=True)
        return lax.dot_general(merged.astype(jnp.bfloat16), weights_buf[offset, slot],
                               (((1,), (1,)), ((), ())), preferred_element_type=jnp.float32)

    def chunk_copy(offset, chunk):
        span = pl.ds(*spans[chunk])
        return pltpu.make_async_remote_copy(
            src_ref=part_ref.at[offset, span], dst_ref=arrived_ref.at[offset, span],
            send_sem=send_sem.at[offset, chunk], recv_sem=recv_sem.at[offset, chunk],
            device_id=place(target(offset)), device_id_type=pl.DeviceIdType.MESH)

    def meta_copy(offset):
        return pltpu.make_async_remote_copy(
            src_ref=meta.at[offset], dst_ref=arrived_meta_ref.at[offset],
            send_sem=meta_send_sem.at[offset], recv_sem=meta_recv_sem.at[offset],
            device_id=place(target(offset)), device_id_type=pl.DeviceIdType.MESH)

    own_meta = pltpu.make_async_copy(meta.at[reach], arrived_meta_ref.at[reach], own_sem)

    def store_slots(offset, chunk):
        begin, size = spans[chunk]

        def one_slot(slot, carry):
            part_ref[offset, slot] = product(offset, slot)
            return carry

        weight_load(offset, chunk).wait()
        lax.fori_loop(begin, begin + size, one_slot, 0, unroll=2 if size % 2 == 0 else 1)

    def send_chunk(chunk, index):
        offset = flow_offset(index)
        store_slots(offset, chunk)
        chunk_copy(offset, chunk).start()
        if chunk == 0:
            meta_copy(offset).start()

    store_slots(2 * reach, 0)
    repeat(0, num_off, lambda offset: meta_load(offset).wait())
    pl.semaphore_wait(barrier, greeted)
    chunk_copy(2 * reach, 0).start()
    meta_copy(2 * reach).start()
    own_meta.start()
    steps(outer, lambda step: column_vote(step, x).start())
    for chunk in range(len(first_spans)):
        repeat(1 if chunk == 0 else 0, 2 * reach,
               lambda index, chunk=chunk: send_chunk(chunk, index))
        if chunk == min(1, len(first_spans) - 1):
            steps(outer, lambda step: column_vote(
                step, lax.rem(x - step + outer, outer)).wait())
            row_votes[y] = jnp.min(column_votes[:, 0, :], axis=0, keepdims=True)
            steps(inner, lambda step: row_vote(step, y).start())
    for chunk in range(len(first_spans), len(spans)):
        repeat(0, 2 * reach, lambda index, chunk=chunk: store_slots(flow_offset(index), chunk))

    def own_slot(slot, carry):
        own_ref[slot] = product(reach, slot)
        return carry

    own_load().wait()
    lax.fori_loop(0, slots, own_slot, 0, unroll=2)
    steps(inner, lambda step: row_vote(step, lax.rem(y - step + inner, inner)).wait())
    agreed = jnp.min(row_votes[:, 0, :], axis=0, keepdims=True)
    pick_ref[0] = jnp.min(jnp.where((agreed > 0) & (lane <= classes), lane, classes))
    own_meta.wait()
    repeat(0, 2 * reach, lambda index: meta_copy(flow_offset(index)).wait())
    for chunk in range(len(first_spans)):
        repeat(0, 2 * reach, lambda index, chunk=chunk: chunk_copy(
            flow_offset(index), chunk).wait())


def rest_kernel(axes, sizes, classes, group, first, half, parts, part_ref, arrived_ref, relay,
                base_send, base_recv, send_sem, recv_sem, pass_send, pass_recv,
                fwd_send, fwd_recv):
    num_off, slots = part_ref.shape[0], part_ref.shape[1]
    reach = num_off // 2
    outer, inner = sizes
    count = outer * inner
    x, y = lax.axis_index(axes[0]), lax.axis_index(axes[1])
    me = x * inner + y
    batch = (half - first) // 2
    piece = (slots - half) // parts

    def place(there):
        return (there // inner, lax.rem(there, inner))

    def shifted(device, offset):
        return lax.rem(device + offset - reach + count, count)

    def origin(offset):
        return lax.rem(me - offset + reach + count, count)

    def beside(part):
        return flip(x, part, outer)

    def remote(src, dst, send, recv, device):
        return pltpu.make_async_remote_copy(
            src_ref=src, dst_ref=dst, send_sem=send, recv_sem=recv,
            device_id=device, device_id_type=pl.DeviceIdType.MESH)

    def member(device):
        return (device if classes == count else lax.rem(device, classes)) == group

    def heavy(source, goal):
        return member(source) | member(goal)

    def near(source, goal):
        return source // CORES == goal // CORES

    def hot(source, offset):
        goal = shifted(source, offset)
        return heavy(source, goal) & jnp.logical_not(near(source, goal))

    def close(source, offset):
        goal = shifted(source, offset)
        return heavy(source, goal) & near(source, goal)

    def repeat(begin, end, act):
        def one(step, carry):
            act(step)
            return carry

        lax.fori_loop(begin, end, one, 0)

    def each_flow(act):
        def one(index):
            away = reach - index // 2
            act(jnp.where(lax.rem(index, 2) == 0, reach + away, reach - away))

        repeat(0, 2 * reach, one)

    def each_part(act):
        repeat(1, parts, act)

    anyone = (lax.rem(x + 1, outer), y)

    def toward(offset):
        return place(shifted(me, offset))

    def span(offset, begin, size, send, recv, device):
        return remote(part_ref.at[offset, pl.ds(begin, size)],
                      arrived_ref.at[offset, pl.ds(begin - first, size)],
                      send, recv, device)

    def base(offset, step, device=anyone):
        size = slots - first if group is None else batch
        return span(offset, first + step * batch, size, base_send.at[offset, step],
                    base_recv.at[offset, step], device)

    def direct(offset, device=anyone):
        return span(offset, half, piece, send_sem.at[offset], recv_sem.at[offset], device)

    def whole(offset, device=anyone):
        return span(offset, half, slots - half, send_sem.at[offset], recv_sem.at[offset],
                    device)

    def detour(offset, part, device=anyone):
        return remote(part_ref.at[offset, pl.ds(half + part * piece, piece)],
                      relay.at[offset, part], pass_send.at[offset, part],
                      pass_recv.at[offset, part], device)

    def forward(offset, part, device=anyone):
        return remote(relay.at[offset, part],
                      arrived_ref.at[offset, pl.ds(half - first + part * piece, piece)],
                      fwd_send.at[offset, part], fwd_recv.at[offset, part], device)

    barrier = pltpu.get_barrier_semaphore()

    def greet(device, inc=1):
        pl.semaphore_signal(barrier, inc=inc, device_id=device,
                            device_id_type=pl.DeviceIdType.MESH)

    each_flow(lambda offset: greet(place(shifted(me, offset))))
    if group is None:
        pl.semaphore_wait(barrier, 2 * reach)
        each_flow(lambda offset: base(offset, 0, toward(offset)).start())
        each_flow(lambda offset: base(offset, 0).wait())
        return

    def greet_flow(index, total):
        away = reach - index // 2
        offset = jnp.where(lax.rem(index, 2) == 0, reach + away, reach - away)
        begun = origin(offset)
        here, there = hot(me, offset), hot(begun, offset)

        def greet_part(part, total):
            source = beside(part) * inner + y
            middleman = hot(source, offset)

            @pl.when(here | middleman)
            def _():
                greet((beside(part), y))

            @pl.when(middleman)
            def _():
                greet(place(shifted(source, offset)))

            @pl.when(there)
            def _():
                greet((flip(begun // inner, part, outer), lax.rem(begun, inner)))

            return (total + jnp.where(here | middleman, 1, 0) + jnp.where(middleman, 1, 0)
                    + jnp.where(there, 1, 0))

        return lax.fori_loop(1, parts, greet_part, total)

    pl.semaphore_wait(barrier, lax.fori_loop(0, 2 * reach, greet_flow, 2 * reach))

    def start_hot(offset):
        @pl.when(hot(me, offset))
        def _():
            each_part(lambda part: detour(offset, part, (beside(part), y)).start())
            direct(offset, toward(offset)).start()

        @pl.when(close(me, offset))
        def _():
            whole(offset, toward(offset)).start()

    def middle(offset, act):
        def one(part):
            source = beside(part) * inner + y

            @pl.when(hot(source, offset))
            def _():
                act(offset, part, source)

        each_part(one)

    def pass_on(offset, part, source):
        detour(offset, part).wait_recv()
        forward(offset, part, place(shifted(source, offset))).start()

    def finish(offset):
        @pl.when(close(me, offset))
        def _():
            whole(offset).wait_send()

        @pl.when(close(origin(offset), offset))
        def _():
            whole(offset).wait_recv()

        @pl.when(hot(me, offset))
        def _():
            direct(offset).wait_send()
            each_part(lambda part: detour(offset, part).wait_send())

        @pl.when(hot(origin(offset), offset))
        def _():
            direct(offset).wait_recv()
            each_part(lambda part: forward(offset, part).wait_recv())

        middle(offset, lambda offset, part, source: forward(offset, part).wait_send())

    def batch_step(step):
        each_flow(lambda offset: base(offset, step, toward(offset)).start())

        @pl.when(step == 0)
        def _():
            each_flow(lambda offset: middle(offset, pass_on))

    each_flow(start_hot)
    repeat(0, 2, batch_step)
    each_flow(finish)
    repeat(0, 2, lambda step: each_flow(lambda offset: base(offset, step).wait()))


def settle_kernel(meta_ref, own_ref, low_ref, high_ref, out_ref, meta, total, out_buf,
                  load_sem, out_sem):
    num_off, first = low_ref.shape[0], low_ref.shape[1]
    reach = num_off // 2
    num_kinds, num_steps = out_ref.shape[0], out_ref.shape[1]
    blocks, _, block_rows = total.shape
    load = pltpu.make_async_copy(meta_ref, meta, load_sem)
    load.start()

    def clear(block, carry):
        total[block] = jnp.zeros_like(total[block])
        return carry

    lax.fori_loop(0, blocks, clear, 0, unroll=4)
    load.wait()

    def add_pair(offset, slot, end, source, shift):
        lone = slot + 1 >= end
        other = jnp.where(lone, slot, slot + 1)
        row, next_row = meta[offset, 0, 0, slot], meta[offset, 0, 0, other]
        value, next_value = source(slot - shift), source(other - shift)
        old, next_old = total[row], total[next_row]
        new = old + value
        kept = jnp.where(row == next_row, new, next_old)
        total[row] = new
        total[next_row] = jnp.where(lone, kept, kept + next_value)

    def add_all(offset, begin, end, source, shift):
        def one(pair, carry):
            add_pair(offset, begin + 2 * pair, end, source, shift)
            return carry

        lax.fori_loop(0, (end - begin + 1) // 2, one, 0)

    def one_flow(offset, carry):
        live = meta[offset, 1, 0, 0]

        @pl.when(offset != reach)
        def _():
            add_all(offset, 0, jnp.minimum(live, first), lambda slot: low_ref[offset, slot], 0)
            add_all(offset, first, jnp.maximum(live, first),
                    lambda slot: high_ref[offset, slot], first)

        return carry

    lax.fori_loop(0, num_off, one_flow, 0)
    add_all(reach, 0, meta[reach, 1, 0, 0], lambda slot: own_ref[slot], 0)

    per_cut = blocks // OUT_CUTS

    def store(cut):
        size = per_cut * block_rows
        lanes = pl.ds(pl.multiple_of(cut * size, size), size)
        return pltpu.make_async_copy(
            out_buf.at[:, :, lanes], out_ref.at[:, :, lanes], out_sem.at[cut])

    def one_cut(cut, carry):
        def one_block(block, carry):
            lanes = pl.ds(pl.multiple_of(block * block_rows, block_rows), block_rows)
            out_buf[:, :, lanes] = total[block].reshape(num_kinds, num_steps, block_rows)
            return carry

        lax.fori_loop(0, per_cut, lambda step, carry: one_block(cut * per_cut + step, carry), 0,
                      unroll=4)
        store(cut).start()
        return carry

    def end_cut(cut, carry):
        store(cut).wait()
        return carry

    lax.fori_loop(0, OUT_CUTS, one_cut, 0)
    lax.fori_loop(0, OUT_CUTS, end_cut, 0)


def on_device(axes, sizes, atm_blocks, tile_flux, tile_frac, weights, block_row, block_col,
              send_counts):
    num_steps, num_kinds = tile_flux.shape[0], tile_flux.shape[1]
    num_flux = num_steps * num_kinds
    num_off, slots, block_rows, block_cols = weights.shape[1:]
    tiles = tile_flux.shape[2]
    land_blocks = tile_flux.shape[3] // block_cols
    rows = block_row.transpose(1, 0, 2)
    columns = block_col.transpose(1, 0, 2)
    count = sizes[0] * sizes[1]
    half, first = slots // 2, slots // 4
    parts = 4 if sizes[0] % 4 == 0 else 1
    piece = (slots - half) // parts
    classes = min(count, MAX_CLASSES)

    vmem = pl.BlockSpec(memory_space=pltpu.VMEM)
    smem = pl.BlockSpec(memory_space=pltpu.SMEM)
    hbm = pl.BlockSpec(memory_space=pltpu.HBM)
    dma = pltpu.SemaphoreType.DMA
    part, own, low, arrived_meta, pick = pl.pallas_call(
        functools.partial(exchange_kernel, axes, sizes, classes, first, half),
        out_shape=(
            pltpu.VMEM((num_off, slots, num_flux, block_rows), jnp.float32),
            pltpu.VMEM((slots, num_flux, block_rows), jnp.float32),
            pltpu.VMEM((num_off, first, num_flux, block_rows), jnp.float32),
            pltpu.VMEM((num_off, 2, 1, slots), jnp.int32),
            jax.ShapeDtypeStruct((1,), jnp.int32),
        ),
        in_specs=[hbm, hbm, smem, smem, hbm, hbm],
        out_specs=(vmem, vmem, vmem, vmem, smem),
        scratch_shapes=[
            pltpu.VMEM((land_blocks, num_steps, num_kinds, tiles, block_cols), tile_flux.dtype),
            pltpu.VMEM((land_blocks, tiles, block_cols), tile_frac.dtype),
            pltpu.VMEM(weights.shape[1:], weights.dtype),
            pltpu.VMEM((num_off, 2, 1, slots), jnp.int32),
            pltpu.VMEM((sizes[0], 1, LANES), jnp.int32),
            pltpu.VMEM((sizes[1], 1, LANES), jnp.int32),
            dma((land_blocks,)),
            dma((land_blocks,)),
            dma((num_off, slots)),
            dma((num_off,)),
            dma,
            dma((num_off, first)),
            dma((num_off, first)),
            dma((num_off,)),
            dma((num_off,)),
            dma((sizes[0],)),
            dma((sizes[0],)),
            dma((sizes[1],)),
            dma((sizes[1],)),
        ],
        compiler_params=pltpu.CompilerParams(collective_id=0, has_side_effects=True,
                                             vmem_limit_bytes=55 * 2**20),
        name="exchange",
    )(tile_flux, tile_frac, columns, send_counts, rows, weights[0])

    def settle(arrived_meta, own, low, high):
        return pl.pallas_call(
            settle_kernel,
            out_shape=jax.ShapeDtypeStruct((num_kinds, num_steps, atm_blocks * block_rows),
                                           jnp.float32),
            in_specs=[vmem] * 4,
            out_specs=hbm,
            scratch_shapes=[
                pltpu.SMEM((num_off, 2, 1, slots), jnp.int32),
                pltpu.VMEM((atm_blocks, num_flux, block_rows), jnp.float32),
                pltpu.VMEM((num_kinds, num_steps, atm_blocks * block_rows), jnp.float32),
                dma,
                dma((OUT_CUTS,)),
            ],
            compiler_params=pltpu.CompilerParams(vmem_limit_bytes=16 * 2**20),
            name="settle",
        )(arrived_meta, own, low, high)

    def rest(group):
        def call(part, arrived_meta, own, low):
            high = pl.pallas_call(
                functools.partial(rest_kernel, axes, sizes, classes, group, first, half, parts),
                out_shape=pltpu.VMEM((num_off, slots - first, num_flux, block_rows),
                                     jnp.float32),
                in_specs=[vmem],
                out_specs=vmem,
                scratch_shapes=[
                    pltpu.VMEM((num_off, parts, piece, num_flux, block_rows), jnp.float32),
                ] + [dma((num_off, 2))] * 2 + [dma((num_off,))] * 2 + [dma((num_off, parts))] * 4,
                compiler_params=pltpu.CompilerParams(
                    collective_id=classes + 1 if group is None else 1 + group,
                    has_side_effects=True, vmem_limit_bytes=16 * 2**20),
                name="rest",
            )(part)
            return settle(arrived_meta, own, low, high)
        return call

    groups = list(range(classes)) + [None]
    out = lax.switch(pick[0], [rest(group) for group in groups],
                     part, arrived_meta, own, low)
    return out.transpose(1, 0, 2)


def solution(mesh):
    axes = ("gx", "gy")
    sizes = (mesh.shape["gx"], mesh.shape["gy"])
    return jax.shard_map(
        functools.partial(on_device, axes, sizes, AB_DEV),
        mesh=mesh,
        in_specs=(
            P(None, None, None, ("gx", "gy")),
            P(None, ("gx", "gy")),
            P(("gx", "gy"), None, None, None, None),
            P(("gx", "gy"), None, None),
            P(("gx", "gy"), None, None),
            P(("gx", "gy"), None),
        ),
        out_specs=P(None, None, ("gx", "gy")),
        check_vma=False,
    )
```
